256 devices in a mesh: groups: 2 (over y), ctx: 32 (over z, core), head: 4 (over x).
Axes of the slice: x: 4, y: 2, z: 16, core: 2. Of those that a mesh axis runs over, the one named last changes fastest.
The devices are a block of a 4x16x16 slice.
Arguments:
- query: bfloat16 [8, 64, 32, 128], P('groups', 'head'), parts along dimension 0
- key_cache: bfloat16 [8, 65536, 8, 128], P('groups', 'ctx', 'head'), parts along dimension 0
- value_cache: bfloat16 [8, 65536, 8, 128], P('groups', 'ctx', 'head'), parts along dimension 0, may hold values from -6 to 6
- new_key: bfloat16 [8, 8, 32, 128], P('groups', 'head'), parts along dimension 0, may hold values from -9 to 9
- new_value: bfloat16 [8, 8, 32, 128], P('groups', 'head'), parts along dimension 0, may hold values from -6 to 6
- lengths: int32 [8], P('groups'), parts along dimension 0, may hold values from 256 to 65536, as said below
- out_weight: bfloat16 [8192, 8192], P('head', 'ctx'), may hold values from -0.0625 to 0.0625
Outputs:
- projected: float32 [8, 32, 8192], P('groups', None, 'ctx'), parts along dimension 0
The draws below stay inside these ranges and needn't reach their ends.
There are 2 independent parts, one for each index of `groups`. The reference program is written for one: setup_inputs(seed, part) draws one part's arguments, and reference() takes and returns one part's arrays. A program takes and returns all parts, laid end to end along the dimension named above; an argument that names none is the same for every part. Nothing has to cross between parts.
Inputs may be any that keep to these rules, and one draw needn't show every extreme that they name: `lengths`: multiples of 256; in every draw exactly one sequence has length 65536, the others less.
All inputs are finite; a program needn't handle non-finite values.
Results may differ from the reference program's by a relative error of at most 0.003.
Values sent between devices are 32-bit elements; how exact they have to be, the bound alone decides.
No kernel may reach another device: no remote copies, remote signals or barrier semaphores. Data moves between devices by JAX's collectives and lax.ppermute only.
A program may use at most 128 MiB of HBM per device.

```python
import math
import jax
import jax.numpy as jnp
from jax import lax

QH = 64
KVH = 8
HD = 128
D = 8192
SEQS = 4
CTX_DEV = 2048
DRAFT = 32
BLOCK = 256
CTX = 65536
N_CTX = 32


def plant_table(key):
    group_size = QH // KVH
    planted = jax.random.normal(jax.random.fold_in(key, 11), (SEQS, 2 * group_size, KVH, HD), jnp.float32)
    return planted


def draw_key_cache(key, part):
    group_size = QH // KVH
    planted = plant_table(key)
    remainder = jax.random.normal(jax.random.fold_in(key, 12), (SEQS, CTX - 2 * group_size, KVH, HD), jnp.float32)
    return jnp.concatenate((planted, remainder), axis=1).astype(jnp.bfloat16)


def draw_query(key, part):
    baseline = 3.0 * jnp.clip(jax.random.normal(jax.random.fold_in(key, 21), (SEQS, QH, DRAFT, HD), jnp.float32), -6.0, 6.0)
    return baseline.astype(jnp.bfloat16)


def draw_lengths(key, part):
    block_count = CTX // BLOCK
    picked = jax.random.randint(jax.random.fold_in(key, 1), (SEQS,), 1, block_count)
    full_seq = jax.random.randint(jax.random.fold_in(key, 2), (), 0, SEQS)
    picked = jnp.where(jnp.arange(SEQS) == full_seq, block_count, picked)
    return (picked * BLOCK).astype(jnp.int32)


def level_of(stream_key, extent, pieces, smallest, high):
    level = 1.0
    for axis_at, parts in pieces:
        heights = jax.random.uniform(jax.random.fold_in(jax.random.fold_in(stream_key, 6), axis_at), (parts,), jnp.float32, smallest / len(pieces), high / len(pieces))
        level = level * jnp.repeat(jnp.exp(heights), extent[axis_at] // parts).reshape((-1,) + (1,) * (len(extent) - 1 - axis_at))
    return level


def normal_values(key, dims, width, reach, split=(), kind=jnp.bfloat16):
    result = width * jax.random.normal(key, dims, jnp.float32)
    if split:
        result = result * level_of(key, dims, split, -0.22, 0.18)
    return jnp.clip(result, -reach, reach).astype(kind)


def setup_inputs(seed: int = 0, part: int = 0) -> dict:
    splits = jax.random.split(jax.random.key(seed), 8)
    part_keys = jax.random.split(jax.random.fold_in(splits[7], part), 8)
    query = draw_query(jax.random.fold_in(jax.random.fold_in(splits[7], part), 71), part)
    key_cache = draw_key_cache(jax.random.fold_in(jax.random.fold_in(splits[7], part), 71), part)
    value_cache = normal_values(part_keys[2], (SEQS, CTX, KVH, HD), 1.0, 6.0, ((1, 32), (2, 4)))
    new_key = normal_values(part_keys[3], (SEQS, KVH, DRAFT, HD), 1.5, 9.0, ((1, 4),))
    new_value = normal_values(part_keys[4], (SEQS, KVH, DRAFT, HD), 1.0, 6.0, ((1, 4),))
    lengths = draw_lengths(jax.random.fold_in(jax.random.fold_in(splits[7], part), 71), part)
    out_weight = normal_values(splits[6], (QH * HD, D), (QH * HD) ** -0.5, 0.0625, ((0, 4), (1, 32)))
    return dict(query=query, key_cache=key_cache, value_cache=value_cache, new_key=new_key, new_value=new_value, lengths=lengths, out_weight=out_weight)


very_low = -1e+30

def reference(query, key_cache, value_cache, new_key, new_value, lengths, out_weight):
    seq_count, q_count, draft_len, head_dim = query.shape
    kv_count = key_cache.shape[2]
    group_rows = q_count // kv_count * draft_len
    scaling = 1.0 / math.sqrt(head_dim)
    grouped = query.reshape(seq_count, kv_count, group_rows, head_dim).astype(jnp.float32)

    def block_stats(block_index):
        offset = (block_index * CTX_DEV).astype(jnp.int32)
        key_block = lax.dynamic_slice_in_dim(key_cache, offset, CTX_DEV, 1).astype(jnp.float32)
        value_block = lax.dynamic_slice_in_dim(value_cache, offset, CTX_DEV, 1).astype(jnp.float32)
        scores = jnp.einsum('sgrd,stgd->sgrt', grouped, key_block) * scaling
        position = offset + jnp.arange(CTX_DEV, dtype=jnp.int32)
        usable = (position[None, :] < lengths[:, None])[:, None, None, :]
        masked = jnp.where(usable, scores, very_low)
        block_top = lax.optimization_barrier(jnp.max(masked, axis=-1))
        weights = jnp.where(usable, jnp.exp(masked - block_top[..., None]), 0.0).astype(jnp.bfloat16)
        widened = weights.astype(jnp.float32)
        return (block_top, lax.optimization_barrier(jnp.sum(widened, axis=-1)), jnp.einsum('sgrt,stgd->sgrd', widened, value_block))
    tops, sums_all, numer_all = lax.map(block_stats, jnp.arange(N_CTX, dtype=jnp.int32))
    global_top = lax.optimization_barrier(jnp.max(tops, axis=0))
    factor = jnp.exp(tops - global_top)
    totals = lax.optimization_barrier(jnp.sum(sums_all * factor, axis=0))
    numerators = lax.optimization_barrier(jnp.sum(numer_all * factor[..., None], axis=0))
    own_scores = jnp.einsum('sgrd,sgjd->sgrj', grouped, new_key.astype(jnp.float32)) * scaling
    row_index = jnp.arange(group_rows) % draft_len
    causal = jnp.arange(draft_len)[None, :] <= row_index[:, None]
    own_scores = jnp.where(causal, own_scores, very_low)
    overall = jnp.maximum(global_top, lax.optimization_barrier(jnp.max(own_scores, axis=-1)))
    carried = jnp.exp(global_top - overall)
    fresh_weights = jnp.where(causal, jnp.exp(own_scores - overall[..., None]), 0.0)
    denominator = totals * carried + lax.optimization_barrier(jnp.sum(fresh_weights, axis=-1))
    numerators = numerators * carried[..., None] + jnp.einsum('sgrj,sgjd->sgrd', fresh_weights, new_value.astype(jnp.float32))
    attended = (numerators / denominator[..., None]).reshape(seq_count, q_count, draft_len, head_dim)
    attended = jnp.transpose(attended, (0, 2, 1, 3)).reshape(seq_count * draft_len, q_count * head_dim).astype(jnp.bfloat16)
    projected = jnp.dot(attended, out_weight, preferred_element_type=jnp.float32)
    return projected.reshape(seq_count, draft_len, -1)
```

```python
import functools
import math

import jax
import jax.numpy as jnp
from jax import lax
from jax.experimental import pallas as pl
from jax.experimental.pallas import tpu as pltpu
from jax.sharding import PartitionSpec as P

very_low = -1e30
page = 256
radix = 4
stat_rows = 8

VMEM = pltpu.VMEM
f32 = jnp.float32
bf16 = jnp.bfloat16


def stats(top, total):
    row = lax.broadcasted_iota(jnp.int32, (stat_rows, top.shape[-1]), 0)
    return jnp.where(row == 0, top, jnp.where(row == 1, total, 0.0))


def contract(a, b, da, db, precision=None):
    return lax.dot_general(
        a, b, (((da,), (db,)), ((), ())), preferred_element_type=f32, precision=precision
    )


def attend_kernel(scaling, lens, info, q_ref, k_ref, v_ref, mine_ref, theirs_ref, s_ref, acc_ref):
    step = pl.program_id(0)
    seq = jnp.bitwise_xor(info[1], step)
    core = info[3]
    rows, head_dim = k_ref.shape
    queries = q_ref.shape[1]
    per_page = 2 * page
    usable = jnp.clip(lens[seq] - info[0], 0, rows // 2)
    pages = usable // page
    factor = scaling * math.log2(math.e)
    d2 = 2 * head_dim

    even_row = lax.broadcasted_iota(jnp.int32, (16, head_dim), 0) % 2 == 0
    pick_even = jnp.where(even_row, 1.0, 0.0).astype(bf16)
    pick_odd = jnp.where(even_row, 0.0, 1.0).astype(bf16)
    qc = jnp.concatenate([q_ref[0], q_ref[1]], axis=1)

    def scores(p, tile):
        k = k_ref[pl.ds(p * per_page, tile), :].reshape(tile // 16, 16, head_dim)
        wide = jnp.concatenate(
            [
                (k * pick_even[None]).reshape(tile, head_dim),
                (k * pick_odd[None]).reshape(tile, head_dim),
            ],
            axis=1,
        )
        s = contract(wide, qc, 1, 1)
        s_ref[pl.ds(p * per_page, tile), :] = s
        return jnp.max(s.reshape(tile // 8, 8, queries), axis=0)

    def tops(most):
        even = lax.broadcasted_iota(jnp.int32, (8, queries), 0) % 2 == 0
        low = jnp.full_like(most, -jnp.inf)
        top0 = jnp.max(jnp.where(even, most, low), axis=0, keepdims=True)
        top1 = jnp.max(jnp.where(even, low, most), axis=0, keepdims=True)
        return top0, top1, jnp.where(even, top0, top1)

    def weighted(p, tile, both):
        s = s_ref[pl.ds(p * per_page, tile), :].reshape(tile // 8, 8, queries)
        w = jnp.exp2((s - both[None]) * factor).reshape(tile, queries).astype(bf16)
        v = v_ref[pl.ds(p * per_page, tile), :].T
        even = lax.broadcasted_iota(jnp.int32, (16, tile), 1) % 2 == 0
        even_lane = jnp.where(even, 1.0, 0.0).astype(bf16)
        odd_lane = jnp.where(even, 0.0, 1.0).astype(bf16)
        first = lax.broadcasted_iota(jnp.int32, (16, tile), 0)
        ones = jnp.where(
            first == 0, even_lane.astype(f32), jnp.where(first == 1, odd_lane.astype(f32), 0.0)
        ).astype(bf16)
        v3 = v.reshape(head_dim // 16, 16, tile)
        wide = jnp.concatenate(
            [
                (v3 * even_lane[None]).reshape(head_dim, tile),
                (v3 * odd_lane[None]).reshape(head_dim, tile),
                ones,
            ],
            axis=0,
        )
        return contract(wide, w, 1, 0)

    def put(acc, top0, top1):
        a0, a1 = acc[:head_dim], acc[head_dim:d2]
        s0 = stats(top0 * scaling, acc[d2 : d2 + 1])
        s1 = stats(top1 * scaling, acc[d2 + 1 : d2 + 2])
        first = core == 0
        mine_ref[:head_dim, :] = jnp.where(first, a0, a1)
        theirs_ref[:head_dim, :] = jnp.where(first, a1, a0)
        mine_ref[head_dim:, :] = jnp.where(first, s0, s1)
        theirs_ref[head_dim:, :] = jnp.where(first, s1, s0)

    whole = rows // per_page

    @pl.when(pages == whole)
    def _():
        most = scores(0, per_page)
        for p in range(1, whole):
            most = jnp.maximum(most, scores(p, per_page))
        top0, top1, both = tops(most)
        acc = weighted(0, per_page, both)
        for p in range(1, whole):
            acc = acc + weighted(p, per_page, both)
        put(acc, top0, top1)

    @pl.when(jnp.logical_and(pages < whole, pages > 0))
    def _():
        most = lax.fori_loop(
            0,
            pages,
            lambda p, m: jnp.maximum(m, scores(p, per_page)),
            jnp.full((8, queries), -jnp.inf, f32),
        )
        top0, top1, both = tops(most)
        acc_ref[...] = jnp.zeros_like(acc_ref)

        def add(p, _):
            acc_ref[...] += weighted(p, per_page, both)
            return _

        lax.fori_loop(0, pages, add, 0)
        put(acc_ref[...], top0, top1)

    @pl.when(pages == 0)
    def _():
        nothing = stats(jnp.full((1, queries), very_low, f32), jnp.zeros((1, queries), f32))
        for ref in (mine_ref, theirs_ref):
            ref[:head_dim, :] = jnp.zeros((head_dim, queries), f32)
            ref[head_dim:, :] = nothing


def attend(query, key_cache, value_cache, lengths, info, scaling):
    seqs, heads, queries, head_dim = query.shape
    rows = key_cache.shape[1]
    out = jax.ShapeDtypeStruct((seqs, head_dim + stat_rows, queries), f32)
    of_seq = lambda k, lens, info: (jnp.bitwise_xor(info[1], k), 0, 0)
    spec = pltpu.PrefetchScalarGridSpec(
        num_scalar_prefetch=2,
        grid=(seqs,),
        in_specs=[
            pl.BlockSpec(
                (None, heads, queries, head_dim),
                lambda k, lens, info: (jnp.bitwise_xor(info[1], k), 0, 0, 0),
            ),
            pl.BlockSpec((None, rows, head_dim), of_seq),
            pl.BlockSpec((None, rows, head_dim), of_seq),
        ],
        out_specs=[
            pl.BlockSpec((None, head_dim + stat_rows, queries), lambda k, lens, info: (k, 0, 0)),
            pl.BlockSpec(
                (None, head_dim + stat_rows, queries),
                lambda k, lens, info: (jnp.bitwise_xor(jnp.bitwise_xor(info[1], info[4]), k), 0, 0),
            ),
        ],
        scratch_shapes=[VMEM((rows, queries), f32), VMEM((2 * head_dim + 16, queries), f32)],
    )
    return pl.pallas_call(
        functools.partial(attend_kernel, scaling),
        grid_spec=spec,
        out_shape=[out, out],
        name="attend",
    )(lengths, info, query, key_cache, value_cache)


def merged(parts, depth):
    tops = [p[depth : depth + 1] for p in parts]
    top = functools.reduce(jnp.maximum, tops)
    shares = [jnp.exp(t - top) for t in tops]
    numer = sum(p[:depth] * e for p, e in zip(parts, shares))
    total = sum(p[depth + 1 : depth + 2] * e for p, e in zip(parts, shares))
    return numer, top, total


def merge_core_kernel(mine_ref, got_ref, *outs):
    depth = mine_ref.shape[1] - stat_rows
    for k, out in enumerate(outs):
        numer, top, total = merged([mine_ref[k], got_ref[k]], depth)
        out[:depth, :] = numer
        out[depth:, :] = stats(top, total)


def merge_near_kernel(info, *refs):
    parts, outs, pieces = refs[:radix], refs[radix:-1], refs[-1]
    depth = parts[0].shape[0] - stat_rows
    numer, top, total = merged([p[...] for p in parts], depth)
    half, lanes = depth // 2, numer.shape[1] // 2
    for a in range(2):
        at = slice(a * lanes, (a + 1) * lanes)
        s = stats(top[:, at], total[:, at])
        for d in range(2):
            pieces[2 * a + d, :half, :] = numer[d * half : (d + 1) * half, at]
            pieces[2 * a + d, half:, :] = s
    for k, out in enumerate(outs):
        out[...] = pieces[jnp.bitwise_xor(info[2], k)]


def finish_kernel(scaling, draft, info, *refs):
    parts, (q_ref, key_ref, value_ref), out = refs[:radix], refs[radix:-1], refs[-1]
    depth = parts[0].shape[0] - stat_rows
    numer, top, total = merged([p[...] for p in parts], depth)
    own = contract(key_ref[...], q_ref[...], 1, 1) * scaling
    at = lax.broadcasted_iota(jnp.int32, own.shape, 0)
    row = lax.broadcasted_iota(jnp.int32, own.shape, 1) % draft
    causal = at <= row
    own = jnp.where(causal, own, very_low)
    overall = jnp.maximum(top, jnp.max(own, axis=0, keepdims=True))
    carried = jnp.exp(top - overall)
    fresh = jnp.where(causal, jnp.exp(own - overall), 0.0)
    denominator = total * carried + jnp.sum(fresh, axis=0, keepdims=True)
    added = contract(value_ref[...].astype(f32), fresh, 0, 0, lax.Precision.HIGHEST)
    added = jnp.where(info[2] % 2 == 0, added[:depth], added[depth:])
    out[...] = ((numer * carried + added) / denominator).astype(bf16).astype(f32)


def collect_kernel(info, *refs):
    parts, out = refs[:-1], refs[-1]
    for k, part in enumerate(parts):
        out[jnp.bitwise_xor(info[2], k)] = part[...]


def project_kernel(draft, info, *refs):
    pieces, (w_ref, out_ref, x_ref) = refs[: 2 * radix], refs[2 * radix :]
    width = x_ref.shape[2]
    for k in range(radix):
        for other in range(2):
            seq = jnp.bitwise_xor(info[4 if other else 1], k)
            where = pl.ds(pl.multiple_of(seq * draft, draft), draft)
            g = jnp.bitwise_xor(info[3], other)
            for a in range(2):
                att = jnp.concatenate([pieces[2 * k + other][2 * a + d] for d in range(2)], axis=0)
                lanes = att.shape[0]
                att = att.T.astype(bf16)
                for h in range(att.shape[0] // draft):
                    col = (a * (att.shape[0] // draft) + h) * lanes
                    x_ref[g, where, col : col + lanes] = att[h * draft : (h + 1) * draft]
    out_ref[...] = sum(contract(x_ref[g], w_ref[g * width : (g + 1) * width, :], 1, 0) for g in range(2))


def whole_vmem(n):
    return [pl.BlockSpec(memory_space=VMEM)] * n


smem = pl.BlockSpec(memory_space=pltpu.SMEM)


def shards(query, key_cache, value_cache, new_key, new_value, lengths, out_weight):
    seqs, q_count, draft, head_dim = query.shape
    ctx_len, heads = key_cache.shape[1], key_cache.shape[2]
    queries = q_count // heads * draft
    scaling = 1.0 / math.sqrt(head_dim)
    n_ctx = lax.axis_size("ctx")
    chips = n_ctx // 2
    far = chips // radix

    def place(z, c):
        u = (z - c * (radix // 2)) % chips
        return u // radix, u % radix

    def chip(b, j, c):
        return (b * radix + j + c * (radix // 2)) % chips

    def pairs(move):
        out = []
        for i in range(n_ctx):
            z, c = i // 2, i % 2
            b, j = place(z, c)
            b2, j2 = move(b, j)
            out.append((i, 2 * chip(b2, j2, c) + c))
        return out

    near_pairs = [pairs(lambda b, j: (b, j ^ k)) for k in range(radix)]
    far_pairs = [pairs(lambda b, j: (b ^ k, j)) for k in range(far)]
    core_pairs = [(i, i ^ 1) for i in range(n_ctx)]
    swap = lambda x: lax.ppermute(x, "ctx", core_pairs)
    to_near = lambda x, k: lax.ppermute(x, "ctx", near_pairs[k])
    to_far = lambda x, k: lax.ppermute(x, "ctx", far_pairs[k])

    index = lax.axis_index("ctx")
    core = index % 2
    block, spot = place(index // 2, core)
    partner_spot = place(index // 2, 1 - core)[1]
    info = jnp.stack([index * ctx_len, spot, block, core, partner_spot]).astype(jnp.int32)

    grouped = query.reshape(seqs, heads, queries, head_dim)
    mine, theirs = attend(
        grouped,
        key_cache.reshape(seqs, ctx_len * heads, head_dim),
        value_cache.reshape(seqs, ctx_len * heads, head_dim),
        lengths,
        info,
        scaling,
    )
    got = swap(theirs)
    chunk = jax.ShapeDtypeStruct((head_dim + stat_rows, queries), f32)
    chunks = pl.pallas_call(
        merge_core_kernel,
        in_specs=whole_vmem(2),
        out_specs=whole_vmem(radix),
        out_shape=[chunk] * radix,
        name="merge_core",
    )(mine, got)
    chunks = [chunks[0]] + [to_near(chunks[k], k) for k in range(1, radix)]
    piece_shape = (head_dim // 2 + stat_rows, queries // 2)
    piece = jax.ShapeDtypeStruct(piece_shape, f32)
    pieces = pl.pallas_call(
        merge_near_kernel,
        in_specs=[smem] + whole_vmem(radix),
        out_specs=whole_vmem(far),
        out_shape=[piece] * far,
        scratch_shapes=[VMEM((4, *piece_shape), f32)],
        name="merge_near",
    )(info, *chunks)
    order = (2, 1, 3)
    moved = {k: to_far(pieces[k], k) for k in order}
    pieces = [pieces[0]] + [moved[k] for k in range(1, far)]
    att_shape = (head_dim // 2, queries // 2)
    picked = pltpu.PrefetchScalarGridSpec(
        num_scalar_prefetch=1,
        grid=(1,),
        in_specs=[pl.BlockSpec(piece_shape, lambda i, info: (0, 0))] * far
        + [
            pl.BlockSpec(
                (None, None, queries // 2, head_dim),
                lambda i, info: (info[1], info[3], info[2] // 2, 0),
            )
        ]
        + [
            pl.BlockSpec(
                (None, None, draft, head_dim), lambda i, info: (info[1], info[3], 0, 0)
            )
        ]
        * 2,
        out_specs=pl.BlockSpec(att_shape, lambda i, info: (0, 0)),
    )
    att = pl.pallas_call(
        functools.partial(finish_kernel, scaling, draft),
        grid_spec=picked,
        out_shape=jax.ShapeDtypeStruct(att_shape, f32),
        name="finish",
    )(info, *pieces, grouped, new_key, new_value)
    moved = {k: to_far(att, k) for k in order}
    block_att = pl.pallas_call(
        collect_kernel,
        in_specs=[smem] + whole_vmem(far),
        out_specs=pl.BlockSpec(memory_space=VMEM),
        out_shape=jax.ShapeDtypeStruct((far, *att_shape), f32),
        name="collect",
    )(info, att, *[moved[k] for k in range(1, far)])
    near = [block_att] + [to_near(block_att, k) for k in range(1, radix)]
    everything = []
    for part in near:
        everything += [part, swap(part)]
    width = out_weight.shape[1]
    partial_out = pl.pallas_call(
        functools.partial(project_kernel, draft),
        in_specs=[smem] + whole_vmem(2 * radix + 1),
        out_specs=pl.BlockSpec(memory_space=VMEM),
        out_shape=jax.ShapeDtypeStruct((seqs * draft, width), f32),
        scratch_shapes=[VMEM((heads, seqs * draft, out_weight.shape[0] // heads), bf16)],
        name="project",
    )(info, *everything, out_weight)
    n_head = lax.axis_size("head")
    turned = [
        lax.ppermute(partial_out, "head", [(i, (i + k) % n_head) for i in range(n_head)])
        for k in range(1, n_head)
    ]
    return sum(turned, partial_out).reshape(seqs, draft, width)


def solution(mesh):
    placed = (
        P("groups", "head", None, None),
        P("groups", "ctx", "head", None),
        P("groups", "ctx", "head", None),
        P("groups", "head", None, None),
        P("groups", "head", None, None),
        P("groups"),
        P("head", "ctx"),
    )
    return jax.shard_map(
        shards, mesh=mesh, in_specs=placed, out_specs=P("groups", None, "ctx"), check_vma=False
    )
```

```python
import functools
import math

import jax
import jax.numpy as jnp
from jax import lax
from jax.experimental import pallas as pl
from jax.experimental.pallas import tpu as pltpu
from jax.sharding import PartitionSpec as P

very_low = -1e30
page = 256
radix = 4
stat_rows = 8

VMEM = pltpu.VMEM
f32 = jnp.float32
bf16 = jnp.bfloat16


def stats(top, total):
    row = lax.broadcasted_iota(jnp.int32, (stat_rows, top.shape[-1]), 0)
    return jnp.where(row == 0, top, jnp.where(row == 1, total, 0.0))


def contract(a, b, da, db, precision=None):
    return lax.dot_general(
        a, b, (((da,), (db,)), ((), ())), preferred_element_type=f32, precision=precision
    )


def attend_kernel(scaling, lens, info, q_ref, k_ref, v_ref, mine_ref, theirs_ref, s_ref, acc_ref):
    step = pl.program_id(0)
    seq = jnp.bitwise_xor(info[1], step)
    core = info[3]
    rows, head_dim = k_ref.shape
    queries = q_ref.shape[1]
    per_page = 2 * page
    usable = jnp.clip(lens[seq] - info[0], 0, rows // 2)
    pages = usable // page
    factor = scaling * math.log2(math.e)
    d2 = 2 * head_dim

    even_row = lax.broadcasted_iota(jnp.int32, (16, head_dim), 0) % 2 == 0
    pick_even = jnp.where(even_row, 1.0, 0.0).astype(bf16)
    pick_odd = jnp.where(even_row, 0.0, 1.0).astype(bf16)
    qc = jnp.concatenate([q_ref[0], q_ref[1]], axis=1)

    def scores(p, tile):
        k = k_ref[pl.ds(p * per_page, tile), :].reshape(tile // 16, 16, head_dim)
        wide = jnp.concatenate(
            [
                (k * pick_even[None]).reshape(tile, head_dim),
                (k * pick_odd[None]).reshape(tile, head_dim),
            ],
            axis=1,
        )
        s = contract(wide, qc, 1, 1)
        s_ref[pl.ds(p * per_page, tile), :] = s
        return jnp.max(s.reshape(tile // 8, 8, queries), axis=0)

    def tops(most):
        even = lax.broadcasted_iota(jnp.int32, (8, queries), 0) % 2 == 0
        low = jnp.full_like(most, -jnp.inf)
        top0 = jnp.max(jnp.where(even, most, low), axis=0, keepdims=True)
        top1 = jnp.max(jnp.where(even, low, most), axis=0, keepdims=True)
        return top0, top1, jnp.where(even, top0, top1)

    def weighted(p, tile, both):
        s = s_ref[pl.ds(p * per_page, tile), :].reshape(tile // 8, 8, queries)
        w = jnp.exp2((s - both[None]) * factor).reshape(tile, queries).astype(bf16)
        v = v_ref[pl.ds(p * per_page, tile), :].T
        even = lax.broadcasted_iota(jnp.int32, (16, tile), 1) % 2 == 0
        even_lane = jnp.where(even, 1.0, 0.0).astype(bf16)
        odd_lane = jnp.where(even, 0.0, 1.0).astype(bf16)
        first = lax.broadcasted_iota(jnp.int32, (16, tile), 0)
        ones = jnp.where(
            first == 0, even_lane.astype(f32), jnp.where(first == 1, odd_lane.astype(f32), 0.0)
        ).astype(bf16)
        v3 = v.reshape(head_dim // 16, 16, tile)
        wide = jnp.concatenate(
            [
                (v3 * even_lane[None]).reshape(head_dim, tile),
                (v3 * odd_lane[None]).reshape(head_dim, tile),
                ones,
            ],
            axis=0,
        )
        return contract(wide, w, 1, 0)

    def put(acc, top0, top1):
        a0, a1 = acc[:head_dim], acc[head_dim:d2]
        s0 = stats(top0 * scaling, acc[d2 : d2 + 1])
        s1 = stats(top1 * scaling, acc[d2 + 1 : d2 + 2])
        first = core == 0
        mine_ref[:head_dim, :] = jnp.where(first, a0, a1)
        theirs_ref[:head_dim, :] = jnp.where(first, a1, a0)
        mine_ref[head_dim:, :] = jnp.where(first, s0, s1)
        theirs_ref[head_dim:, :] = jnp.where(first, s1, s0)

    whole = rows // per_page

    @pl.when(pages == whole)
    def _():
        most = scores(0, per_page)
        for p in range(1, whole):
            most = jnp.maximum(most, scores(p, per_page))
        top0, top1, both = tops(most)
        acc = weighted(0, per_page, both)
        for p in range(1, whole):
            acc = acc + weighted(p, per_page, both)
        put(acc, top0, top1)

    @pl.when(jnp.logical_and(pages < whole, pages > 0))
    def _():
        most = lax.fori_loop(
            0,
            pages,
            lambda p, m: jnp.maximum(m, scores(p, per_page)),
            jnp.full((8, queries), -jnp.inf, f32),
        )
        top0, top1, both = tops(most)
        acc_ref[...] = jnp.zeros_like(acc_ref)

        def add(p, _):
            acc_ref[...] += weighted(p, per_page, both)
            return _

        lax.fori_loop(0, pages, add, 0)
        put(acc_ref[...], top0, top1)

    @pl.when(pages == 0)
    def _():
        nothing = stats(jnp.full((1, queries), very_low, f32), jnp.zeros((1, queries), f32))
        for ref in (mine_ref, theirs_ref):
            ref[:head_dim, :] = jnp.zeros((head_dim, queries), f32)
            ref[head_dim:, :] = nothing


def attend(query, key_cache, value_cache, lengths, info, scaling):
    seqs, heads, queries, head_dim = query.shape
    rows = key_cache.shape[1]
    out = jax.ShapeDtypeStruct((seqs, head_dim + stat_rows, queries), f32)
    of_seq = lambda k, lens, info: (jnp.bitwise_xor(info[1], k), 0, 0)
    spec = pltpu.PrefetchScalarGridSpec(
        num_scalar_prefetch=2,
        grid=(seqs,),
        in_specs=[
            pl.BlockSpec(
                (None, heads, queries, head_dim),
                lambda k, lens, info: (jnp.bitwise_xor(info[1], k), 0, 0, 0),
            ),
            pl.BlockSpec((None, rows, head_dim), of_seq),
            pl.BlockSpec((None, rows, head_dim), of_seq),
        ],
        out_specs=[
            pl.BlockSpec((None, head_dim + stat_rows, queries), lambda k, lens, info: (k, 0, 0)),
            pl.BlockSpec(
                (None, head_dim + stat_rows, queries),
                lambda k, lens, info: (jnp.bitwise_xor(jnp.bitwise_xor(info[1], info[4]), k), 0, 0),
            ),
        ],
        scratch_shapes=[VMEM((rows, queries), f32), VMEM((2 * head_dim + 16, queries), f32)],
    )
    return pl.pallas_call(
        functools.partial(attend_kernel, scaling),
        grid_spec=spec,
        out_shape=[out, out],
        name="attend",
        compiler_params=limit(24),
    )(lengths, info, *(pltpu.with_memory_space_constraint(x, pltpu.HBM) for x in (query, key_cache, value_cache)))


def merged(parts, depth):
    tops = [p[depth : depth + 1] for p in parts]
    top = functools.reduce(jnp.maximum, tops)
    shares = [jnp.exp(t - top) for t in tops]
    numer = sum(p[:depth] * e for p, e in zip(parts, shares))
    total = sum(p[depth + 1 : depth + 2] * e for p, e in zip(parts, shares))
    return numer, top, total


def merge_core_kernel(mine_ref, got_ref, *outs):
    depth = mine_ref.shape[1] - stat_rows
    for k, out in enumerate(outs):
        numer, top, total = merged([mine_ref[k], got_ref[k]], depth)
        out[:depth, :] = numer
        out[depth:, :] = stats(top, total)


def merge_near_kernel(info, *refs):
    parts, outs, pieces = refs[:radix], refs[radix:-1], refs[-1]
    depth = parts[0].shape[0] - stat_rows
    numer, top, total = merged([p[...] for p in parts], depth)
    half, lanes = depth // 2, numer.shape[1] // 2
    for a in range(2):
        at = slice(a * lanes, (a + 1) * lanes)
        s = stats(top[:, at], total[:, at])
        for d in range(2):
            pieces[2 * a + d, :half, :] = numer[d * half : (d + 1) * half, at]
            pieces[2 * a + d, half:, :] = s
    for k, out in enumerate(outs):
        out[...] = pieces[jnp.bitwise_xor(info[2], k)]


def finish_kernel(scaling, draft, info, *refs):
    parts, (q_ref, key_ref, value_ref), out = refs[:radix], refs[radix:-1], refs[-1]
    depth = parts[0].shape[0] - stat_rows
    numer, top, total = merged([p[...] for p in parts], depth)
    own = contract(key_ref[...], q_ref[...], 1, 1) * scaling
    at = lax.broadcasted_iota(jnp.int32, own.shape, 0)
    row = lax.broadcasted_iota(jnp.int32, own.shape, 1) % draft
    causal = at <= row
    own = jnp.where(causal, own, very_low)
    overall = jnp.maximum(top, jnp.max(own, axis=0, keepdims=True))
    carried = jnp.exp(top - overall)
    fresh = jnp.where(causal, jnp.exp(own - overall), 0.0)
    denominator = total * carried + jnp.sum(fresh, axis=0, keepdims=True)
    added = contract(value_ref[...].astype(f32), fresh, 0, 0, lax.Precision.HIGHEST)
    added = jnp.where(info[2] % 2 == 0, added[:depth], added[depth:])
    out[...] = ((numer * carried + added) / denominator).astype(bf16).astype(f32)


def collect_kernel(info, *refs):
    parts, out = refs[:-1], refs[-1]
    for k, part in enumerate(parts):
        out[jnp.bitwise_xor(info[2], k)] = part[...]


def project_kernel(draft, info, *refs):
    pieces, (w_ref, out_ref, x_ref) = refs[: 2 * radix], refs[2 * radix :]
    width = x_ref.shape[2]
    for k in range(radix):
        for other in range(2):
            seq = jnp.bitwise_xor(info[4 if other else 1], k)
            where = pl.ds(pl.multiple_of(seq * draft, draft), draft)
            g = jnp.bitwise_xor(info[3], other)
            for a in range(2):
                att = jnp.concatenate([pieces[2 * k + other][2 * a + d] for d in range(2)], axis=0)
                lanes = att.shape[0]
                att = att.T.astype(bf16)
                for h in range(att.shape[0] // draft):
                    col = (a * (att.shape[0] // draft) + h) * lanes
                    x_ref[g, where, col : col + lanes] = att[h * draft : (h + 1) * draft]
    out_ref[...] = sum(contract(x_ref[g], w_ref[g * width : (g + 1) * width, :], 1, 0) for g in range(2))


def whole_vmem(n):
    return [pl.BlockSpec(memory_space=VMEM)] * n


def limit(mib):
    return pltpu.CompilerParams(vmem_limit_bytes=mib * 2**20)


smem = pl.BlockSpec(memory_space=pltpu.SMEM)


def shards(query, key_cache, value_cache, new_key, new_value, lengths, out_weight):
    seqs, q_count, draft, head_dim = query.shape
    ctx_len, heads = key_cache.shape[1], key_cache.shape[2]
    queries = q_count // heads * draft
    scaling = 1.0 / math.sqrt(head_dim)
    n_ctx = lax.axis_size("ctx")
    chips = n_ctx // 2
    far = chips // radix

    def place(z, c):
        u = (z - c * (radix // 2)) % chips
        return u // radix, u % radix

    def chip(b, j, c):
        return (b * radix + j + c * (radix // 2)) % chips

    def pairs(move):
        out = []
        for i in range(n_ctx):
            z, c = i // 2, i % 2
            b, j = place(z, c)
            b2, j2 = move(b, j)
            out.append((i, 2 * chip(b2, j2, c) + c))
        return out

    near_pairs = [pairs(lambda b, j: (b, j ^ k)) for k in range(radix)]
    far_pairs = [pairs(lambda b, j: (b ^ k, j)) for k in range(far)]
    core_pairs = [(i, i ^ 1) for i in range(n_ctx)]
    swap = lambda x: lax.ppermute(x, "ctx", core_pairs)
    to_near = lambda x, k: lax.ppermute(x, "ctx", near_pairs[k])
    to_far = lambda x, k: lax.ppermute(x, "ctx", far_pairs[k])

    index = lax.axis_index("ctx")
    core = index % 2
    block, spot = place(index // 2, core)
    partner_spot = place(index // 2, 1 - core)[1]
    info = jnp.stack([index * ctx_len, spot, block, core, partner_spot]).astype(jnp.int32)

    grouped = query.reshape(seqs, heads, queries, head_dim)
    mine, theirs = attend(
        grouped,
        key_cache.reshape(seqs, ctx_len * heads, head_dim),
        value_cache.reshape(seqs, ctx_len * heads, head_dim),
        lengths,
        info,
        scaling,
    )
    got = swap(theirs)
    chunk = jax.ShapeDtypeStruct((head_dim + stat_rows, queries), f32)
    chunks = pl.pallas_call(
        merge_core_kernel,
        in_specs=whole_vmem(2),
        out_specs=whole_vmem(radix),
        out_shape=[chunk] * radix,
        name="merge_core",
        compiler_params=limit(8),
    )(mine, got)
    chunks = [chunks[0]] + [to_near(chunks[k], k) for k in range(1, radix)]
    piece_shape = (head_dim // 2 + stat_rows, queries // 2)
    piece = jax.ShapeDtypeStruct(piece_shape, f32)
    pieces = pl.pallas_call(
        merge_near_kernel,
        in_specs=[smem] + whole_vmem(radix),
        out_specs=whole_vmem(far),
        out_shape=[piece] * far,
        scratch_shapes=[VMEM((4, *piece_shape), f32)],
        name="merge_near",
        compiler_params=limit(4),
    )(info, *chunks)
    order = (2, 1, 3)
    moved = {k: to_far(pieces[k], k) for k in order}
    pieces = [pieces[0]] + [moved[k] for k in range(1, far)]
    att_shape = (head_dim // 2, queries // 2)
    picked = pltpu.PrefetchScalarGridSpec(
        num_scalar_prefetch=1,
        grid=(1,),
        in_specs=[pl.BlockSpec(piece_shape, lambda i, info: (0, 0))] * far
        + [
            pl.BlockSpec(
                (None, None, queries // 2, head_dim),
                lambda i, info: (info[1], info[3], info[2] // 2, 0),
            )
        ]
        + [
            pl.BlockSpec(
                (None, None, draft, head_dim), lambda i, info: (info[1], info[3], 0, 0)
            )
        ]
        * 2,
        out_specs=pl.BlockSpec(att_shape, lambda i, info: (0, 0)),
    )
    att = pl.pallas_call(
        functools.partial(finish_kernel, scaling, draft),
        grid_spec=picked,
        out_shape=jax.ShapeDtypeStruct(att_shape, f32),
        name="finish",
        compiler_params=limit(4),
    )(info, *pieces, grouped, new_key, new_value)
    moved = {k: to_far(att, k) for k in order}
    block_att = pl.pallas_call(
        collect_kernel,
        in_specs=[smem] + whole_vmem(far),
        out_specs=pl.BlockSpec(memory_space=VMEM),
        out_shape=jax.ShapeDtypeStruct((far, *att_shape), f32),
        name="collect",
        compiler_params=limit(4),
    )(info, att, *[moved[k] for k in range(1, far)])
    near = [block_att] + [to_near(block_att, k) for k in range(1, radix)]
    everything = []
    for part in near:
        everything += [part, swap(part)]
    width = out_weight.shape[1]
    partial_out = pl.pallas_call(
        functools.partial(project_kernel, draft),
        in_specs=[smem] + whole_vmem(2 * radix + 1),
        out_specs=pl.BlockSpec(memory_space=VMEM),
        out_shape=jax.ShapeDtypeStruct((seqs * draft, width), f32),
        scratch_shapes=[VMEM((heads, seqs * draft, out_weight.shape[0] // heads), bf16)],
        name="project",
        compiler_params=limit(8),
    )(info, *everything, out_weight)
    n_head = lax.axis_size("head")
    turned = [
        lax.ppermute(partial_out, "head", [(i, (i + k) % n_head) for i in range(n_head)])
        for k in range(1, n_head)
    ]
    return sum(turned, partial_out).reshape(seqs, draft, width)


def solution(mesh):
    placed = (
        P("groups", "head", None, None),
        P("groups", "ctx", "head", None),
        P("groups", "ctx", "head", None),
        P("groups", "head", None, None),
        P("groups", "head", None, None),
        P("groups"),
        P("head", "ctx"),
    )
    return jax.shard_map(
        shards, mesh=mesh, in_specs=placed, out_specs=P("groups", None, "ctx"), check_vma=False
    )
```

```python
import functools
import math

import jax
import jax.numpy as jnp
from jax import lax
from jax.experimental import pallas as pl
from jax.experimental.pallas import tpu as pltpu
from jax.sharding import PartitionSpec as P


very_low = -1e30
page = 256
radix = 4
stat_rows = 8

VMEM = pltpu.VMEM
f32 = jnp.float32
bf16 = jnp.bfloat16


def stats(top, total):
    row = lax.broadcasted_iota(jnp.int32, (stat_rows, top.shape[-1]), 0)
    return jnp.where(row == 0, top, jnp.where(row == 1, total, 0.0))


def contract(a, b, da, db, precision=None):
    return lax.dot_general(
        a, b, (((da,), (db,)), ((), ())), preferred_element_type=f32, precision=precision
    )


def attend_kernel(scaling, order, lens, info, q_ref, k_ref, v_ref, mine_ref, theirs_ref, s_ref, acc_ref):
    seq = jnp.bitwise_xor(info[1], order(pl.program_id(0)))
    core = info[3]
    rows, head_dim = k_ref.shape
    queries = q_ref.shape[1]
    per_page = 2 * page
    usable = jnp.clip(lens[seq] - info[0], 0, rows // 2)
    pages = usable // page
    factor = scaling * math.log2(math.e)
    d2 = 2 * head_dim

    even_row = lax.broadcasted_iota(jnp.int32, (16, head_dim), 0) % 2 == 0
    pick_even = jnp.where(even_row, 1.0, 0.0).astype(bf16)
    pick_odd = jnp.where(even_row, 0.0, 1.0).astype(bf16)
    qc = jnp.concatenate([q_ref[0], q_ref[1]], axis=1)

    def scores(p, tile):
        k = k_ref[pl.ds(p * per_page, tile), :].reshape(tile // 16, 16, head_dim)
        wide = jnp.concatenate(
            [
                (k * pick_even[None]).reshape(tile, head_dim),
                (k * pick_odd[None]).reshape(tile, head_dim),
            ],
            axis=1,
        )
        s = contract(wide, qc, 1, 1)
        s_ref[pl.ds(p * per_page, tile), :] = s
        return jnp.max(s.reshape(tile // 8, 8, queries), axis=0)

    def tops(most):
        even = lax.broadcasted_iota(jnp.int32, (8, queries), 0) % 2 == 0
        low = jnp.full_like(most, -jnp.inf)
        top0 = jnp.max(jnp.where(even, most, low), axis=0, keepdims=True)
        top1 = jnp.max(jnp.where(even, low, most), axis=0, keepdims=True)
        return top0, top1, jnp.where(even, top0, top1)

    def weighted(p, tile, both):
        s = s_ref[pl.ds(p * per_page, tile), :].reshape(tile // 8, 8, queries)
        w = jnp.exp2((s - both[None]) * factor).reshape(tile, queries).astype(bf16)
        v = v_ref[pl.ds(p * per_page, tile), :].T
        even = lax.broadcasted_iota(jnp.int32, (16, tile), 1) % 2 == 0
        even_lane = jnp.where(even, 1.0, 0.0).astype(bf16)
        odd_lane = jnp.where(even, 0.0, 1.0).astype(bf16)
        first = lax.broadcasted_iota(jnp.int32, (16, tile), 0)
        ones = jnp.where(
            first == 0, even_lane.astype(f32), jnp.where(first == 1, odd_lane.astype(f32), 0.0)
        ).astype(bf16)
        v3 = v.reshape(head_dim // 16, 16, tile)
        wide = jnp.concatenate(
            [
                (v3 * even_lane[None]).reshape(head_dim, tile),
                (v3 * odd_lane[None]).reshape(head_dim, tile),
                ones,
            ],
            axis=0,
        )
        return contract(wide, w, 1, 0)

    def put(acc, top0, top1):
        a0, a1 = acc[:head_dim], acc[head_dim:d2]
        s0 = stats(top0 * scaling, acc[d2 : d2 + 1])
        s1 = stats(top1 * scaling, acc[d2 + 1 : d2 + 2])
        first = core == 0
        mine_ref[:head_dim, :] = jnp.where(first, a0, a1)
        theirs_ref[:head_dim, :] = jnp.where(first, a1, a0)
        mine_ref[head_dim:, :] = jnp.where(first, s0, s1)
        theirs_ref[head_dim:, :] = jnp.where(first, s1, s0)

    whole = rows // per_page

    @pl.when(pages == whole)
    def _():
        most = scores(0, per_page)
        for p in range(1, whole):
            most = jnp.maximum(most, scores(p, per_page))
        top0, top1, both = tops(most)
        acc = weighted(0, per_page, both)
        for p in range(1, whole):
            acc = acc + weighted(p, per_page, both)
        put(acc, top0, top1)

    @pl.when(jnp.logical_and(pages < whole, pages > 0))
    def _():
        most = lax.fori_loop(
            0,
            pages,
            lambda p, m: jnp.maximum(m, scores(p, per_page)),
            jnp.full((8, queries), -jnp.inf, f32),
        )
        top0, top1, both = tops(most)
        acc_ref[...] = jnp.zeros_like(acc_ref)

        def add(p, _):
            acc_ref[...] += weighted(p, per_page, both)
            return _

        lax.fori_loop(0, pages, add, 0)
        put(acc_ref[...], top0, top1)

    @pl.when(pages == 0)
    def _():
        nothing = stats(jnp.full((1, queries), very_low, f32), jnp.zeros((1, queries), f32))
        for ref in (mine_ref, theirs_ref):
            ref[:head_dim, :] = jnp.zeros((head_dim, queries), f32)
            ref[head_dim:, :] = nothing


def attend(query, key_cache, value_cache, lengths, info, scaling, order, steps):
    _, heads, queries, head_dim = query.shape
    rows = key_cache.shape[1]
    block = (None, head_dim + stat_rows, queries)
    out = jax.ShapeDtypeStruct((steps, *block[1:]), f32)
    of_seq = lambda k, lens, info: (jnp.bitwise_xor(info[1], order(k)), 0, 0)
    spec = pltpu.PrefetchScalarGridSpec(
        num_scalar_prefetch=2,
        grid=(steps,),
        in_specs=[
            pl.BlockSpec(
                (None, heads, queries, head_dim),
                lambda k, lens, info: (jnp.bitwise_xor(info[1], order(k)), 0, 0, 0),
            ),
            pl.BlockSpec((None, rows, head_dim), of_seq),
            pl.BlockSpec((None, rows, head_dim), of_seq),
        ],
        out_specs=[pl.BlockSpec(block, lambda k, lens, info: (k, 0, 0))] * 2,
        scratch_shapes=[VMEM((rows, queries), f32), VMEM((2 * head_dim + 16, queries), f32)],
    )
    cost = pl.CostEstimate(
        flops=8 * steps * rows * queries * head_dim,
        transcendentals=steps * rows * queries,
        bytes_accessed=4 * steps * rows * head_dim,
    )
    in_hbm = [pltpu.with_memory_space_constraint(x, pltpu.HBM) for x in (query, key_cache, value_cache)]
    return pl.pallas_call(
        functools.partial(attend_kernel, scaling, order),
        grid_spec=spec,
        out_shape=[out, out],
        name="attend",
        compiler_params=limit(24),
        cost_estimate=cost,
    )(lengths, info, *in_hbm)


def merged(parts, depth):
    tops = [p[depth : depth + 1] for p in parts]
    top = functools.reduce(jnp.maximum, tops)
    shares = [jnp.exp(t - top) for t in tops]
    numer = sum(p[:depth] * e for p, e in zip(parts, shares))
    total = sum(p[depth + 1 : depth + 2] * e for p, e in zip(parts, shares))
    return numer, top, total


def merge_core_kernel(mine_ref, got_ref, *outs):
    depth = mine_ref.shape[1] - stat_rows
    for k, out in enumerate(outs):
        numer, top, total = merged([mine_ref[k], got_ref[k]], depth)
        out[:depth, :] = numer
        out[depth:, :] = stats(top, total)


def merge_near_kernel(info, *refs):
    parts, outs, pieces = refs[:radix], refs[radix:-1], refs[-1]
    depth = parts[0].shape[0] - stat_rows
    numer, top, total = merged([p[...] for p in parts], depth)
    half, lanes = depth // 2, numer.shape[1] // 2
    for a in range(2):
        at = slice(a * lanes, (a + 1) * lanes)
        s = stats(top[:, at], total[:, at])
        for d in range(2):
            pieces[2 * a + d, :half, :] = numer[d * half : (d + 1) * half, at]
            pieces[2 * a + d, half:, :] = s
    for k, out in enumerate(outs):
        out[...] = pieces[jnp.bitwise_xor(info[2], k)]


def finish_kernel(scaling, draft, info, *refs):
    parts, (q_ref, key_ref, value_ref), out = refs[:radix], refs[radix:-1], refs[-1]
    depth = parts[0].shape[0] - stat_rows
    numer, top, total = merged([p[...] for p in parts], depth)
    own = contract(key_ref[...], q_ref[...], 1, 1) * scaling
    at = lax.broadcasted_iota(jnp.int32, own.shape, 0)
    row = lax.broadcasted_iota(jnp.int32, own.shape, 1) % draft
    causal = at <= row
    own = jnp.where(causal, own, very_low)
    overall = jnp.maximum(top, jnp.max(own, axis=0, keepdims=True))
    carried = jnp.exp(top - overall)
    fresh = jnp.where(causal, jnp.exp(own - overall), 0.0)
    denominator = total * carried + jnp.sum(fresh, axis=0, keepdims=True)
    added = contract(value_ref[...].astype(f32), fresh, 0, 0, lax.Precision.HIGHEST)
    added = jnp.where(info[2] % 2 == 0, added[:depth], added[depth:])
    out[...] = ((numer * carried + added) / denominator).astype(bf16).astype(f32)


def collect_kernel(info, *refs):
    parts, out = refs[:-1], refs[-1]
    for k, part in enumerate(parts):
        out[jnp.bitwise_xor(info[2], k)] = part[...]


def project_kernel(draft, info, *refs):
    pieces, (w_ref, out_ref, x_ref) = refs[:-3], refs[-3:]
    width = x_ref.shape[2]
    for i, piece in enumerate(pieces):
        k, other = i // 2, i % 2
        g = jnp.bitwise_xor(info[3], other)
        for a in range(2):
            att = jnp.concatenate([piece[2 * a + d] for d in range(2)], axis=0)
            lanes, rows = att.shape
            att = att.T.astype(bf16)
            for h in range(rows // draft):
                col = (a * (rows // draft) + h) * lanes
                x_ref[g, k * draft : (k + 1) * draft, col : col + lanes] = att[h * draft : (h + 1) * draft]
    out_ref[...] = sum(contract(x_ref[g], w_ref[g * width : (g + 1) * width, :], 1, 0) for g in range(2))


def total_kernel(draft, n, info, *refs):
    parts, out = refs[:-1], refs[-1]
    for half in range(len(parts) // n):
        whole = sum(p[...] for p in parts[half * n : (half + 1) * n])
        count = whole.shape[0] // draft
        for i in range(count):
            seq = jnp.bitwise_xor(info[1], half * count + i)
            out[seq] = whole[i * draft : (i + 1) * draft]


def whole_vmem(n):
    return [pl.BlockSpec(memory_space=VMEM)] * n


def limit(mib):
    return pltpu.CompilerParams(vmem_limit_bytes=mib * 2**20)


smem = pl.BlockSpec(memory_space=pltpu.SMEM)


def step(query, key_cache, value_cache, new_key, new_value, lengths, out_weight):
    seqs, q_count, draft, head_dim = query.shape
    ctx_len, heads = key_cache.shape[1], key_cache.shape[2]
    queries = q_count // heads * draft
    scaling = 1.0 / math.sqrt(head_dim)
    n_ctx = lax.axis_size("ctx")
    chips = n_ctx // 2
    far = chips // radix

    def place(z, c):
        return (z - c * (radix // 2)) % chips // radix, z % radix

    def chip(b, j, c):
        shift = c * (radix // 2)
        return (b * radix + shift + (j - shift) % radix) % chips

    def pairs(move):
        out = []
        for i in range(n_ctx):
            z, c = i // 2, i % 2
            b, j = place(z, c)
            b2, j2 = move(b, j)
            out.append((i, 2 * chip(b2, j2, c) + c))
        return out

    near_pairs = [pairs(lambda b, j: (b, j ^ k)) for k in range(radix)]
    far_pairs = [pairs(lambda b, j: (b ^ k, j)) for k in range(far)]
    core_pairs = [(i, i ^ 1) for i in range(n_ctx)]

    swap = lambda x: lax.ppermute(x, "ctx", core_pairs)
    to_near = lambda x, k: lax.ppermute(x, "ctx", near_pairs[k])
    to_far = lambda x, k: lax.ppermute(x, "ctx", far_pairs[k])

    index = lax.axis_index("ctx")
    core = index % 2
    block, spot = place(index // 2, core)
    info = jnp.stack([index * ctx_len, spot, block, core]).astype(jnp.int32)

    grouped = query.reshape(seqs, heads, queries, head_dim)
    keys = key_cache.reshape(seqs, ctx_len * heads, head_dim)
    values = value_cache.reshape(seqs, ctx_len * heads, head_dim)
    chunk = jax.ShapeDtypeStruct((head_dim + stat_rows, queries), f32)
    half_seqs = seqs // 2
    gate = info
    chunks = {}
    for half in range(2):
        order = lambda k, half=half: seqs - 1 - half * half_seqs - k
        mine, theirs = attend(grouped, keys, values, lengths, gate, scaling, order, half_seqs)
        got = swap(theirs)
        found = pl.pallas_call(
            merge_core_kernel,
            in_specs=whole_vmem(2),
            out_specs=whole_vmem(half_seqs),
            out_shape=[chunk] * half_seqs,
            name="merge_core",
            compiler_params=limit(8),
        )(mine, got)
        gate, *found = lax.optimization_barrier((info, *found))
        for k, x in enumerate(found):
            chunks[order(k)] = to_near(x, order(k)) if order(k) else x
    chunks = [chunks[k] for k in range(radix)]
    piece_shape = (head_dim // 2 + stat_rows, queries // 2)
    piece = jax.ShapeDtypeStruct(piece_shape, f32)
    pieces = pl.pallas_call(
        merge_near_kernel,
        in_specs=[smem] + whole_vmem(radix),
        out_specs=whole_vmem(far),
        out_shape=[piece] * far,
        scratch_shapes=[VMEM((4, *piece_shape), f32)],
        name="merge_near",
        compiler_params=limit(4),
    )(info, *chunks)
    order = (2, 1, 3)
    moved = {k: to_far(pieces[k], k) for k in order}
    pieces = [pieces[0]] + [moved[k] for k in range(1, far)]
    att_shape = (head_dim // 2, queries // 2)
    picked = pltpu.PrefetchScalarGridSpec(
        num_scalar_prefetch=1,
        grid=(1,),
        in_specs=[pl.BlockSpec(piece_shape, lambda i, info: (0, 0))] * far
        + [
            pl.BlockSpec(
                (None, None, queries // 2, head_dim),
                lambda i, info: (info[1], info[3], info[2] // 2, 0),
            )
        ]
        + [
            pl.BlockSpec(
                (None, None, draft, head_dim), lambda i, info: (info[1], info[3], 0, 0)
            )
        ]
        * 2,
        out_specs=pl.BlockSpec(att_shape, lambda i, info: (0, 0)),
    )
    att = pl.pallas_call(
        functools.partial(finish_kernel, scaling, draft),
        grid_spec=picked,
        out_shape=jax.ShapeDtypeStruct(att_shape, f32),
        name="finish",
        compiler_params=limit(4),
    )(info, *pieces, grouped, new_key, new_value)
    moved = {k: to_far(att, k) for k in order}
    block_att = pl.pallas_call(
        collect_kernel,
        in_specs=[smem] + whole_vmem(far),
        out_specs=pl.BlockSpec(memory_space=VMEM),
        out_shape=jax.ShapeDtypeStruct((far, *att_shape), f32),
        name="collect",
        compiler_params=limit(4),
    )(info, att, *[moved[k] for k in range(1, far)])
    near = [block_att] + [to_near(block_att, k) for k in range(1, radix)]
    width = out_weight.shape[1]
    n_head = lax.axis_size("head")
    parts = []
    for half in range(2):
        pieces = []
        for k in range(half * half_seqs, (half + 1) * half_seqs):
            pieces += [near[k], swap(near[k])]
        partial_out = pl.pallas_call(
            functools.partial(project_kernel, draft),
            in_specs=[smem] + whole_vmem(len(pieces) + 1),
            out_specs=pl.BlockSpec(memory_space=VMEM),
            out_shape=jax.ShapeDtypeStruct((half_seqs * draft, width), f32),
            scratch_shapes=[VMEM((heads, half_seqs * draft, out_weight.shape[0] // heads), bf16)],
            name="project",
            compiler_params=limit(8),
        )(info, *pieces, out_weight)
        parts.append(partial_out)
        for k in range(1, n_head):
            moves = [(i, (i + k) % n_head) for i in range(n_head)]
            parts.append(lax.ppermute(partial_out, "head", moves))
    return pl.pallas_call(
        functools.partial(total_kernel, draft, n_head),
        in_specs=[smem] + whole_vmem(len(parts)),
        out_specs=pl.BlockSpec(memory_space=VMEM),
        out_shape=jax.ShapeDtypeStruct((seqs, draft, width), f32),
        name="total",
        compiler_params=limit(4),
    )(info, *parts)


def solution(mesh):
    placed = (
        P("groups", "head", None, None),
        P("groups", "ctx", "head", None),
        P("groups", "ctx", "head", None),
        P("groups", "head", None, None),
        P("groups", "head", None, None),
        P("groups"),
        P("head", "ctx"),
    )
    return jax.shard_map(
        step, mesh=mesh, in_specs=placed, out_specs=P("groups", None, "ctx"), check_vma=False
    )
```

```python
import functools
import math

import jax
import jax.numpy as jnp
from jax import lax
from jax.experimental import pallas as pl
from jax.experimental.pallas import tpu as pltpu
from jax.sharding import PartitionSpec as P


very_low = -1e30
page = 256
radix = 4
stat_rows = 8

VMEM = pltpu.VMEM
f32 = jnp.float32
bf16 = jnp.bfloat16


def stats(top, total):
    row = lax.broadcasted_iota(jnp.int32, (stat_rows, top.shape[-1]), 0)
    return jnp.where(row == 0, top, jnp.where(row == 1, total, 0.0))


def contract(a, b, da, db, precision=None):
    return lax.dot_general(
        a, b, (((da,), (db,)), ((), ())), preferred_element_type=f32, precision=precision
    )


def attend_kernel(scaling, order, lens, info, q_ref, k_ref, v_ref, mine_ref, theirs_ref, s_ref, acc_ref):
    seq = jnp.bitwise_xor(info[1], order(pl.program_id(0)))
    core = info[2]
    rows, head_dim = k_ref.shape
    queries = q_ref.shape[1]
    per_page = 2 * page
    usable = jnp.clip(lens[seq] - info[0], 0, rows // 2)
    pages = usable // page
    factor = scaling * math.log2(math.e)
    d2 = 2 * head_dim

    even_row = lax.broadcasted_iota(jnp.int32, (16, head_dim), 0) % 2 == 0
    pick_even = jnp.where(even_row, 1.0, 0.0).astype(bf16)
    pick_odd = jnp.where(even_row, 0.0, 1.0).astype(bf16)
    qc = jnp.concatenate([q_ref[0], q_ref[1]], axis=1)

    def scores(p, tile):
        k = k_ref[pl.ds(p * per_page, tile), :].reshape(tile // 16, 16, head_dim)
        wide = jnp.concatenate(
            [
                (k * pick_even[None]).reshape(tile, head_dim),
                (k * pick_odd[None]).reshape(tile, head_dim),
            ],
            axis=1,
        )
        s = contract(wide, qc, 1, 1)
        s_ref[pl.ds(p * per_page, tile), :] = s
        return jnp.max(s.reshape(tile // 8, 8, queries), axis=0)

    def tops(most):
        even = lax.broadcasted_iota(jnp.int32, (8, queries), 0) % 2 == 0
        low = jnp.full_like(most, -jnp.inf)
        top0 = jnp.max(jnp.where(even, most, low), axis=0, keepdims=True)
        top1 = jnp.max(jnp.where(even, low, most), axis=0, keepdims=True)
        return top0, top1, jnp.where(even, top0, top1)

    def weighted(p, tile, both):
        s = s_ref[pl.ds(p * per_page, tile), :].reshape(tile // 8, 8, queries)
        w = jnp.exp2((s - both[None]) * factor).reshape(tile, queries).astype(bf16)
        v = v_ref[pl.ds(p * per_page, tile), :].T
        even = lax.broadcasted_iota(jnp.int32, (16, tile), 1) % 2 == 0
        even_lane = jnp.where(even, 1.0, 0.0).astype(bf16)
        odd_lane = jnp.where(even, 0.0, 1.0).astype(bf16)
        first = lax.broadcasted_iota(jnp.int32, (16, tile), 0)
        ones = jnp.where(
            first == 0, even_lane.astype(f32), jnp.where(first == 1, odd_lane.astype(f32), 0.0)
        ).astype(bf16)
        v3 = v.reshape(head_dim // 16, 16, tile)
        wide = jnp.concatenate(
            [
                (v3 * even_lane[None]).reshape(head_dim, tile),
                (v3 * odd_lane[None]).reshape(head_dim, tile),
                ones,
            ],
            axis=0,
        )
        return contract(wide, w, 1, 0)

    def put(acc, top0, top1):
        a0, a1 = acc[:head_dim], acc[head_dim:d2]
        s0 = stats(top0 * scaling, acc[d2 : d2 + 1])
        s1 = stats(top1 * scaling, acc[d2 + 1 : d2 + 2])
        first = core == 0
        mine_ref[:head_dim, :] = jnp.where(first, a0, a1)
        theirs_ref[:head_dim, :] = jnp.where(first, a1, a0)
        mine_ref[head_dim:, :] = jnp.where(first, s0, s1)
        theirs_ref[head_dim:, :] = jnp.where(first, s1, s0)

    whole = rows // per_page

    @pl.when(pages == whole)
    def _():
        most = scores(0, per_page)
        for p in range(1, whole):
            most = jnp.maximum(most, scores(p, per_page))
        top0, top1, both = tops(most)
        acc = weighted(0, per_page, both)
        for p in range(1, whole):
            acc = acc + weighted(p, per_page, both)
        put(acc, top0, top1)

    @pl.when(jnp.logical_and(pages < whole, pages > 0))
    def _():
        most = lax.fori_loop(
            0,
            pages,
            lambda p, m: jnp.maximum(m, scores(p, per_page)),
            jnp.full((8, queries), -jnp.inf, f32),
        )
        top0, top1, both = tops(most)
        acc_ref[...] = jnp.zeros_like(acc_ref)

        def add(p, _):
            acc_ref[...] += weighted(p, per_page, both)
            return _

        lax.fori_loop(0, pages, add, 0)
        put(acc_ref[...], top0, top1)

    @pl.when(pages == 0)
    def _():
        nothing = stats(jnp.full((1, queries), very_low, f32), jnp.zeros((1, queries), f32))
        for ref in (mine_ref, theirs_ref):
            ref[:head_dim, :] = jnp.zeros((head_dim, queries), f32)
            ref[head_dim:, :] = nothing


def attend(query, key_cache, value_cache, lengths, info, scaling, order, steps):
    _, heads, queries, head_dim = query.shape
    rows = key_cache.shape[1]
    block = (None, head_dim + stat_rows, queries)
    out = jax.ShapeDtypeStruct((steps, *block[1:]), f32)
    of_seq = lambda k, lens, info: (jnp.bitwise_xor(info[1], order(k)), 0, 0)
    spec = pltpu.PrefetchScalarGridSpec(
        num_scalar_prefetch=2,
        grid=(steps,),
        in_specs=[
            pl.BlockSpec(
                (None, heads, queries, head_dim),
                lambda k, lens, info: (jnp.bitwise_xor(info[1], order(k)), 0, 0, 0),
            ),
            pl.BlockSpec((None, rows, head_dim), of_seq),
            pl.BlockSpec((None, rows, head_dim), of_seq),
        ],
        out_specs=[pl.BlockSpec(block, lambda k, lens, info: (k, 0, 0))] * 2,
        scratch_shapes=[VMEM((rows, queries), f32), VMEM((2 * head_dim + 16, queries), f32)],
    )
    cost = pl.CostEstimate(
        flops=8 * steps * rows * queries * head_dim,
        transcendentals=steps * rows * queries,
        bytes_accessed=4 * steps * rows * head_dim,
    )
    in_hbm = [pltpu.with_memory_space_constraint(x, pltpu.HBM) for x in (query, key_cache, value_cache)]
    return pl.pallas_call(
        functools.partial(attend_kernel, scaling, order),
        grid_spec=spec,
        out_shape=[out, out],
        name="attend",
        compiler_params=limit(24),
        cost_estimate=cost,
    )(lengths, info, *in_hbm)


def merged(parts, depth):
    tops = [p[depth : depth + 1] for p in parts]
    top = functools.reduce(jnp.maximum, tops)
    shares = [jnp.exp(t - top) for t in tops]
    numer = sum(p[:depth] * e for p, e in zip(parts, shares))
    total = sum(p[depth + 1 : depth + 2] * e for p, e in zip(parts, shares))
    return numer, top, total


def merge_core_kernel(mine_ref, got_ref, *outs):
    depth = mine_ref.shape[1] - stat_rows
    for k, out in enumerate(outs):
        numer, top, total = merged([mine_ref[k], got_ref[k]], depth)
        out[:depth, :] = numer
        out[depth:, :] = stats(top, total)


def merge_kernel(*refs):
    parts, out = refs[:-1], refs[-1]
    depth = out.shape[0] - stat_rows
    numer, top, total = merged([p[...] for p in parts], depth)
    out[:depth, :] = numer
    out[depth:, :] = stats(top, total)


def finish_kernel(scaling, draft, info, *refs):
    parts, (q_ref, key_ref, value_ref), out = refs[:-4], refs[-4:-1], refs[-1]
    depth = parts[0].shape[0] - stat_rows
    numer, top, total = merged([p[...] for p in parts], depth)
    own = contract(key_ref[...], q_ref[...], 1, 1) * scaling
    at = lax.broadcasted_iota(jnp.int32, own.shape, 0)
    row = lax.broadcasted_iota(jnp.int32, own.shape, 1) % draft
    causal = at <= row
    own = jnp.where(causal, own, very_low)
    overall = jnp.maximum(top, jnp.max(own, axis=0, keepdims=True))
    carried = jnp.exp(top - overall)
    fresh = jnp.where(causal, jnp.exp(own - overall), 0.0)
    denominator = total * carried + jnp.sum(fresh, axis=0, keepdims=True)
    added = contract(value_ref[...].astype(f32), fresh, 0, 0, lax.Precision.HIGHEST)
    out[...] = ((numer * carried + added) / denominator).astype(bf16).astype(f32)


def project_kernel(draft, info, *refs):
    pieces, (w_ref, out_ref, x_ref) = refs[:-3], refs[-3:]
    width = x_ref.shape[2]
    for i, piece in enumerate(pieces):
        k, other = i // 2, i % 2
        g = jnp.bitwise_xor(info[2], other)
        seq = jnp.bitwise_xor(info[1], k)
        at = pl.ds(pl.multiple_of(seq * draft, draft), draft)
        depth, queries = piece.shape
        for a in range(queries // depth):
            att = piece[:, a * depth : (a + 1) * depth].T.astype(bf16)
            for h in range(depth // draft):
                col = (a * (depth // draft) + h) * depth
                x_ref[g, at, col : col + depth] = att[h * draft : (h + 1) * draft]
    out_ref[...] = sum(contract(x_ref[g], w_ref[g * width : (g + 1) * width, :], 1, 0) for g in range(2))


def whole_vmem(n):
    return [pl.BlockSpec(memory_space=VMEM)] * n


def limit(mib):
    return pltpu.CompilerParams(vmem_limit_bytes=mib * 2**20)


smem = pl.BlockSpec(memory_space=pltpu.SMEM)


def step(query, key_cache, value_cache, new_key, new_value, lengths, out_weight):
    seqs, q_count, draft, head_dim = query.shape
    ctx_len, heads = key_cache.shape[1], key_cache.shape[2]
    queries = q_count // heads * draft
    scaling = 1.0 / math.sqrt(head_dim)
    n_ctx = lax.axis_size("ctx")
    chips = n_ctx // 2
    far = chips // radix

    def place(z, c):
        return (z - c * (radix // 2)) % chips // radix, z % radix

    def chip(b, j, c):
        shift = c * (radix // 2)
        return (b * radix + shift + (j - shift) % radix) % chips

    def pairs(move):
        out = []
        for i in range(n_ctx):
            z, c = i // 2, i % 2
            b, j = place(z, c)
            b2, j2 = move(b, j, c)
            out.append((i, 2 * chip(b2, j2, c) + c))
        return out

    def partner(i, n, turn):
        return i ^ 1 if turn == 0 else (((i + 1) % n) ^ 1) - 1 if ((i + 1) % n) ^ 1 else n - 1

    near_pairs = [pairs(lambda b, j, c: (b, j ^ k)) for k in range(radix)]
    far_pairs = [pairs(lambda b, j, c: (partner(b, far, t ^ c), j)) for t in range(2)]
    n_head = lax.axis_size("head")
    head_pairs = [
        [
            (i * n_head + h, i * n_head + partner(h, n_head, t ^ (i % 2)))
            for i in range(n_ctx)
            for h in range(n_head)
        ]
        for t in range(2)
    ]
    core_pairs = [(i, i ^ 1) for i in range(n_ctx)]

    swap = lambda x: lax.ppermute(x, "ctx", core_pairs)
    to_near = lambda x, k: lax.ppermute(x, "ctx", near_pairs[k])
    to_far = lambda x, t: lax.ppermute(x, "ctx", far_pairs[t])
    to_head = lambda x, t: lax.ppermute(x, ("ctx", "head"), head_pairs[t])

    index = lax.axis_index("ctx")
    core = index % 2
    spot = place(index // 2, core)[1]
    info = jnp.stack([index * ctx_len, spot, core]).astype(jnp.int32)

    grouped = query.reshape(seqs, heads, queries, head_dim)
    keys = key_cache.reshape(seqs, ctx_len * heads, head_dim)
    values = value_cache.reshape(seqs, ctx_len * heads, head_dim)
    chunk = jax.ShapeDtypeStruct((head_dim + stat_rows, queries), f32)
    half_seqs = seqs // 2
    gate = info
    chunks = {}
    for half in range(2):
        order = lambda k, half=half: seqs - 1 - half * half_seqs - k
        mine, theirs = attend(grouped, keys, values, lengths, gate, scaling, order, half_seqs)
        got = swap(theirs)
        found = pl.pallas_call(
            merge_core_kernel,
            in_specs=whole_vmem(2),
            out_specs=whole_vmem(half_seqs),
            out_shape=[chunk] * half_seqs,
            name="merge_core",
            compiler_params=limit(8),
        )(mine, got)
        gate, *found = lax.optimization_barrier((info, *found))
        for k, x in enumerate(found):
            chunks[order(k)] = to_near(x, order(k)) if order(k) else x
    chunks = [chunks[k] for k in range(radix)]

    def merge(parts):
        return pl.pallas_call(
            merge_kernel,
            in_specs=whole_vmem(len(parts)),
            out_specs=pl.BlockSpec(memory_space=VMEM),
            out_shape=chunk,
            name="merge",
            compiler_params=limit(4),
        )(*parts)

    found = merge(chunks)
    found = merge([found, to_far(found, 0)])
    parts = [found, to_far(found, 1)]
    att_shape = (head_dim, queries)
    of_spot = lambda i, info: (info[1], info[2], 0, 0)
    picked = pltpu.PrefetchScalarGridSpec(
        num_scalar_prefetch=1,
        grid=(1,),
        in_specs=[pl.BlockSpec(chunk.shape, lambda i, info: (0, 0))] * 2
        + [pl.BlockSpec((None, None, queries, head_dim), of_spot)]
        + [pl.BlockSpec((None, None, draft, head_dim), of_spot)] * 2,
        out_specs=pl.BlockSpec(att_shape, lambda i, info: (0, 0)),
    )
    att = pl.pallas_call(
        functools.partial(finish_kernel, scaling, draft),
        grid_spec=picked,
        out_shape=jax.ShapeDtypeStruct(att_shape, f32),
        name="finish",
        compiler_params=limit(4),
    )(info, *parts, grouped, new_key, new_value)
    near = [att] + [to_near(att, k) for k in range(1, radix)]
    pieces = []
    for part in near:
        pieces += [part, swap(part)]
    width = out_weight.shape[1]
    out = pl.pallas_call(
        functools.partial(project_kernel, draft),
        in_specs=[smem] + whole_vmem(len(pieces) + 1),
        out_specs=pl.BlockSpec(memory_space=VMEM),
        out_shape=jax.ShapeDtypeStruct((seqs * draft, width), f32),
        scratch_shapes=[VMEM((heads, seqs * draft, out_weight.shape[0] // heads), bf16)],
        name="project",
        compiler_params=limit(8),
    )(info, *pieces, out_weight)
    for t in range(2):
        out = out + to_head(out, t)
    return out.reshape(seqs, draft, width)


def solution(mesh):
    placed = (
        P("groups", "head", None, None),
        P("groups", "ctx", "head", None),
        P("groups", "ctx", "head", None),
        P("groups", "head", None, None),
        P("groups", "head", None, None),
        P("groups"),
        P("head", "ctx"),
    )
    return jax.shard_map(
        step, mesh=mesh, in_specs=placed, out_specs=P("groups", None, "ctx"), check_vma=False
    )
```

```python
import functools
import math

import jax
import jax.numpy as jnp
from jax import lax
from jax.experimental import pallas as pl
from jax.experimental.pallas import tpu as pltpu
from jax.sharding import PartitionSpec as P


very_low = -1e30
page = 256
radix = 4
stat_rows = 8

VMEM = pltpu.VMEM
f32 = jnp.float32
bf16 = jnp.bfloat16


def stats(top, total):
    row = lax.broadcasted_iota(jnp.int32, (stat_rows, top.shape[-1]), 0)
    return jnp.where(row == 0, top, jnp.where(row == 1, total, 0.0))


def contract(a, b, da, db, precision=None):
    return lax.dot_general(
        a, b, (((da,), (db,)), ((), ())), preferred_element_type=f32, precision=precision
    )


def attend_kernel(scaling, order, info, q_ref, k_ref, v_ref, mine_ref, theirs_ref, s_ref, acc_ref):
    seq = jnp.bitwise_xor(info[1], order(pl.program_id(0)))
    core = info[2]
    rows, head_dim = k_ref.shape
    queries = q_ref.shape[1]
    per_page = 2 * page
    usable = jnp.clip(info[3 + seq] - info[0], 0, rows // 2)
    pages = usable // page
    factor = scaling * math.log2(math.e)
    d2 = 2 * head_dim

    even_row = lax.broadcasted_iota(jnp.int32, (16, head_dim), 0) % 2 == 0
    pick_even = jnp.where(even_row, 1.0, 0.0).astype(bf16)
    pick_odd = jnp.where(even_row, 0.0, 1.0).astype(bf16)
    qc = jnp.concatenate([q_ref[0], q_ref[1]], axis=1)

    def scores(p, tile):
        k = k_ref[pl.ds(p * per_page, tile), :].reshape(tile // 16, 16, head_dim)
        wide = jnp.concatenate(
            [
                (k * pick_even[None]).reshape(tile, head_dim),
                (k * pick_odd[None]).reshape(tile, head_dim),
            ],
            axis=1,
        )
        s = contract(wide, qc, 1, 1)
        s_ref[pl.ds(p * per_page, tile), :] = s
        return jnp.max(s.reshape(tile // 8, 8, queries), axis=0)

    def tops(most):
        even = lax.broadcasted_iota(jnp.int32, (8, queries), 0) % 2 == 0
        low = jnp.full_like(most, -jnp.inf)
        top0 = jnp.max(jnp.where(even, most, low), axis=0, keepdims=True)
        top1 = jnp.max(jnp.where(even, low, most), axis=0, keepdims=True)
        return top0, top1, jnp.where(even, top0, top1)

    def weighted(p, tile, both):
        s = s_ref[pl.ds(p * per_page, tile), :].reshape(tile // 8, 8, queries)
        w = jnp.exp2((s - both[None]) * factor).reshape(tile, queries).astype(bf16)
        v = v_ref[pl.ds(p * per_page, tile), :].T
        even = lax.broadcasted_iota(jnp.int32, (16, tile), 1) % 2 == 0
        even_lane = jnp.where(even, 1.0, 0.0).astype(bf16)
        odd_lane = jnp.where(even, 0.0, 1.0).astype(bf16)
        first = lax.broadcasted_iota(jnp.int32, (16, tile), 0)
        ones = jnp.where(
            first == 0, even_lane.astype(f32), jnp.where(first == 1, odd_lane.astype(f32), 0.0)
        ).astype(bf16)
        v3 = v.reshape(head_dim // 16, 16, tile)
        wide = jnp.concatenate(
            [
                (v3 * even_lane[None]).reshape(head_dim, tile),
                (v3 * odd_lane[None]).reshape(head_dim, tile),
                ones,
            ],
            axis=0,
        )
        return contract(wide, w, 1, 0)

    def put(acc, top0, top1):
        a0, a1 = acc[:head_dim], acc[head_dim:d2]
        s0 = stats(top0 * scaling, acc[d2 : d2 + 1])
        s1 = stats(top1 * scaling, acc[d2 + 1 : d2 + 2])
        first = core == 0
        mine_ref[:head_dim, :] = jnp.where(first, a0, a1)
        theirs_ref[:head_dim, :] = jnp.where(first, a1, a0)
        mine_ref[head_dim:, :] = jnp.where(first, s0, s1)
        theirs_ref[head_dim:, :] = jnp.where(first, s1, s0)

    whole = rows // per_page

    @pl.when(pages == whole)
    def _():
        most = scores(0, per_page)
        for p in range(1, whole):
            most = jnp.maximum(most, scores(p, per_page))
        top0, top1, both = tops(most)
        acc = weighted(0, per_page, both)
        for p in range(1, whole):
            acc = acc + weighted(p, per_page, both)
        put(acc, top0, top1)

    @pl.when(jnp.logical_and(pages < whole, pages > 0))
    def _():
        most = lax.fori_loop(
            0,
            pages,
            lambda p, m: jnp.maximum(m, scores(p, per_page)),
            jnp.full((8, queries), -jnp.inf, f32),
        )
        top0, top1, both = tops(most)
        acc_ref[...] = jnp.zeros_like(acc_ref)

        def add(p, _):
            acc_ref[...] += weighted(p, per_page, both)
            return _

        lax.fori_loop(0, pages, add, 0)
        put(acc_ref[...], top0, top1)

    @pl.when(pages == 0)
    def _():
        nothing = stats(jnp.full((1, queries), very_low, f32), jnp.zeros((1, queries), f32))
        for ref in (mine_ref, theirs_ref):
            ref[:head_dim, :] = jnp.zeros((head_dim, queries), f32)
            ref[head_dim:, :] = nothing


def attend(query, key_cache, value_cache, info, scaling, order, steps):
    _, heads, queries, head_dim = query.shape
    rows = key_cache.shape[1]
    block = (None, head_dim + stat_rows, queries)
    out = jax.ShapeDtypeStruct((steps, *block[1:]), f32)

    def used(k, info):
        return info[3 + jnp.bitwise_xor(info[1], order(k))] > info[0]

    def of_seq(k, info):
        first = jnp.int32(0)
        for step in reversed(range(1, steps)):
            first = jnp.where(used(step, info), step, first)
        at = jnp.where(used(0, info), 0, first)
        for step in range(1, steps):
            at = jnp.where(jnp.logical_and(k >= step, used(step, info)), step, at)
        return jnp.bitwise_xor(info[1], order(at)), 0, 0

    spec = pltpu.PrefetchScalarGridSpec(
        num_scalar_prefetch=1,
        grid=(steps,),
        in_specs=[
            pl.BlockSpec(
                (None, heads, queries, head_dim),
                lambda k, info: (jnp.bitwise_xor(info[1], order(k)), 0, 0, 0),
            ),
            pl.BlockSpec((None, rows, head_dim), of_seq),
            pl.BlockSpec((None, rows, head_dim), of_seq),
        ],
        out_specs=[pl.BlockSpec(block, lambda k, info: (k, 0, 0))] * 2,
        scratch_shapes=[VMEM((rows, queries), f32), VMEM((2 * head_dim + 16, queries), f32)],
    )
    cost = pl.CostEstimate(
        flops=8 * steps * rows * queries * head_dim,
        transcendentals=steps * rows * queries,
        bytes_accessed=4 * steps * rows * head_dim,
    )
    in_hbm = [pltpu.with_memory_space_constraint(x, pltpu.HBM) for x in (query, key_cache, value_cache)]
    return pl.pallas_call(
        functools.partial(attend_kernel, scaling, order),
        grid_spec=spec,
        out_shape=[out, out],
        name="attend",
        compiler_params=limit(24),
        cost_estimate=cost,
    )(info, *in_hbm)


def merged(parts, depth):
    tops = [p[depth : depth + 1] for p in parts]
    top = functools.reduce(jnp.maximum, tops)
    shares = [jnp.exp(t - top) for t in tops]
    numer = sum(p[:depth] * e for p, e in zip(parts, shares))
    total = sum(p[depth + 1 : depth + 2] * e for p, e in zip(parts, shares))
    return numer, top, total


def merge_core_kernel(mine_ref, got_ref, *outs):
    depth = mine_ref.shape[1] - stat_rows
    for k, out in enumerate(outs):
        numer, top, total = merged([mine_ref[k], got_ref[k]], depth)
        out[:depth, :] = numer
        out[depth:, :] = stats(top, total)


def merge_kernel(*refs):
    parts, out = refs[:-1], refs[-1]
    depth = out.shape[0] - stat_rows
    numer, top, total = merged([p[...] for p in parts], depth)
    out[:depth, :] = numer
    out[depth:, :] = stats(top, total)


def finish_kernel(scaling, draft, info, *refs):
    parts, (q_ref, key_ref, value_ref), out = refs[:-4], refs[-4:-1], refs[-1]
    depth = parts[0].shape[0] - stat_rows
    numer, top, total = merged([p[...] for p in parts], depth)
    own = contract(key_ref[info[1], info[2]], q_ref[info[1], info[2]], 1, 1) * scaling
    at = lax.broadcasted_iota(jnp.int32, own.shape, 0)
    row = lax.broadcasted_iota(jnp.int32, own.shape, 1) % draft
    causal = at <= row
    own = jnp.where(causal, own, very_low)
    overall = jnp.maximum(top, jnp.max(own, axis=0, keepdims=True))
    carried = jnp.exp(top - overall)
    fresh = jnp.where(causal, jnp.exp(own - overall), 0.0)
    denominator = total * carried + jnp.sum(fresh, axis=0, keepdims=True)
    added = contract(value_ref[info[1], info[2]].astype(f32), fresh, 0, 0, lax.Precision.HIGHEST)
    out[...] = ((numer * carried + added) / denominator).astype(bf16).astype(f32)


def project_kernel(draft, info, *refs):
    pieces, (w_ref, out_ref, x_ref) = refs[:-3], refs[-3:]
    width = x_ref.shape[2]
    for i, piece in enumerate(pieces):
        k, other = i // 2, i % 2
        g = jnp.bitwise_xor(info[2], other)
        seq = jnp.bitwise_xor(info[1], k)
        at = pl.ds(pl.multiple_of(seq * draft, draft), draft)
        depth, queries = piece.shape
        for a in range(queries // depth):
            att = piece[:, a * depth : (a + 1) * depth].T.astype(bf16)
            for h in range(depth // draft):
                col = (a * (depth // draft) + h) * depth
                x_ref[g, at, col : col + depth] = att[h * draft : (h + 1) * draft]
    out_ref[...] = sum(contract(x_ref[g], w_ref[g * width : (g + 1) * width, :], 1, 0) for g in range(2))


def whole_vmem(n):
    return [pl.BlockSpec(memory_space=VMEM)] * n


def limit(mib):
    return pltpu.CompilerParams(vmem_limit_bytes=mib * 2**20)


smem = pl.BlockSpec(memory_space=pltpu.SMEM)


def step(query, key_cache, value_cache, new_key, new_value, lengths, out_weight):
    seqs, q_count, draft, head_dim = query.shape
    ctx_len, heads = key_cache.shape[1], key_cache.shape[2]
    queries = q_count // heads * draft
    scaling = 1.0 / math.sqrt(head_dim)
    n_ctx = lax.axis_size("ctx")
    chips = n_ctx // 2
    far = chips // radix

    def place(z, c):
        return (z - c * (radix // 2)) % chips // radix, z % radix

    def chip(b, j, c):
        shift = c * (radix // 2)
        return (b * radix + shift + (j - shift) % radix) % chips

    def pairs(k):
        out = []
        for i in range(n_ctx):
            z, c = divmod(i, 2)
            b, j = place(z, c)
            out.append((i, 2 * chip(b, j ^ k, c) + c))
        return out

    def partner(i, n, turn):
        return i ^ 1 if turn == 0 else (((i + 1) % n) ^ 1) - 1 if ((i + 1) % n) ^ 1 else n - 1

    near_pairs = [pairs(k) for k in range(radix)]
    far_pairs = [
        [
            (i, 2 * (partner(z // radix, far, t ^ c) * radix + z % radix) + c)
            for i in range(n_ctx)
            for z, c in [divmod(i, 2)]
        ]
        for t in range(2)
    ]
    n_head = lax.axis_size("head")
    head_pairs = [
        [
            (i * n_head + h, i * n_head + partner(h, n_head, t ^ (i % 2)))
            for i in range(n_ctx)
            for h in range(n_head)
        ]
        for t in range(2)
    ]
    core_pairs = [(i, i ^ 1) for i in range(n_ctx)]

    swap = lambda x: lax.ppermute(x, "ctx", core_pairs)
    to_near = lambda x, k: lax.ppermute(x, "ctx", near_pairs[k])
    to_far = lambda x, t: lax.ppermute(x, "ctx", far_pairs[t])
    to_head = lambda x, t: lax.ppermute(x, ("ctx", "head"), head_pairs[t])

    index = lax.axis_index("ctx")
    core = index % 2
    spot = place(index // 2, core)[1]
    info = jnp.concatenate([jnp.stack([index * ctx_len, spot, core]).astype(jnp.int32), lengths])

    grouped = query.reshape(seqs, heads, queries, head_dim)
    keys = key_cache.reshape(seqs, ctx_len * heads, head_dim)
    values = value_cache.reshape(seqs, ctx_len * heads, head_dim)
    chunk = jax.ShapeDtypeStruct((head_dim + stat_rows, queries), f32)
    half_seqs = seqs // 2
    gate = info
    chunks = {}
    for half in range(2):
        order = lambda k, half=half: seqs - 1 - half * half_seqs - k
        mine, theirs = attend(grouped, keys, values, gate, scaling, order, half_seqs)
        got = swap(theirs)
        found = pl.pallas_call(
            merge_core_kernel,
            in_specs=whole_vmem(2),
            out_specs=whole_vmem(half_seqs),
            out_shape=[chunk] * half_seqs,
            name="merge_core",
            compiler_params=limit(8),
        )(mine, got)
        gate, *found = lax.optimization_barrier((info, *found))
        for k, x in enumerate(found):
            chunks[order(k)] = to_near(x, order(k)) if order(k) else x
    chunks = [chunks[k] for k in range(radix)]

    def merge(parts):
        return pl.pallas_call(
            merge_kernel,
            in_specs=whole_vmem(len(parts)),
            out_specs=pl.BlockSpec(memory_space=VMEM),
            out_shape=chunk,
            name="merge",
            compiler_params=limit(4),
        )(*parts)

    found = merge(chunks)
    found = merge([found, to_far(found, 0)])
    parts = [found, to_far(found, 1)]
    att = pl.pallas_call(
        functools.partial(finish_kernel, scaling, draft),
        in_specs=[smem] + whole_vmem(5),
        out_specs=pl.BlockSpec(memory_space=VMEM),
        out_shape=jax.ShapeDtypeStruct((head_dim, queries), f32),
        name="finish",
        compiler_params=limit(4),
    )(info, *parts, grouped, new_key, new_value)
    near = [att] + [to_near(att, k) for k in range(1, radix)]
    pieces = []
    for part in near:
        pieces += [part, swap(part)]
    width = out_weight.shape[1]
    out = pl.pallas_call(
        functools.partial(project_kernel, draft),
        in_specs=[smem] + whole_vmem(len(pieces) + 1),
        out_specs=pl.BlockSpec(memory_space=VMEM),
        out_shape=jax.ShapeDtypeStruct((seqs * draft, width), f32),
        scratch_shapes=[VMEM((heads, seqs * draft, out_weight.shape[0] // heads), bf16)],
        name="project",
        compiler_params=limit(8),
    )(info, *pieces, out_weight)
    for t in range(2):
        out = out + to_head(out, t)
    return out.reshape(seqs, draft, width)


def solution(mesh):
    placed = (
        P("groups", "head", None, None),
        P("groups", "ctx", "head", None),
        P("groups", "ctx", "head", None),
        P("groups", "head", None, None),
        P("groups", "head", None, None),
        P("groups"),
        P("head", "ctx"),
    )
    return jax.shard_map(
        step, mesh=mesh, in_specs=placed, out_specs=P("groups", None, "ctx"), check_vma=False
    )
```

```python
import functools
import math

import jax
import jax.numpy as jnp
from jax import lax
from jax.experimental import pallas as pl
from jax.experimental.pallas import tpu as pltpu
from jax.sharding import PartitionSpec as P


very_low = -1e30
page = 256
radix = 4
stat_rows = 8

VMEM = pltpu.VMEM
f32 = jnp.float32
bf16 = jnp.bfloat16


def stats(top, total):
    row = lax.broadcasted_iota(jnp.int32, (stat_rows, top.shape[-1]), 0)
    return jnp.where(row == 0, top, jnp.where(row == 1, total, 0.0))


def contract(a, b, da, db, precision=None):
    return lax.dot_general(
        a, b, (((da,), (db,)), ((), ())), preferred_element_type=f32, precision=precision
    )


def attend_kernel(scaling, order, info, q_hbm, k_hbm, v_hbm, mine_ref, theirs_ref, *scratch):
    q_buf, k_buf, v_buf, s_ref, acc_ref, sems = scratch
    steps = q_buf.shape[0]

    def copies(i):
        seq = jnp.bitwise_xor(info[1], order(i))
        return [
            pltpu.make_async_copy(hbm.at[seq], buf.at[i], sems.at[i, n])
            for n, (hbm, buf) in enumerate(((q_hbm, q_buf), (k_hbm, k_buf), (v_hbm, v_buf)))
        ]

    def usable(i):
        seq = jnp.bitwise_xor(info[1], order(i))
        return jnp.clip(info[3 + seq] - info[0], 0, k_buf.shape[1] // 2)

    for i in range(steps):

        @pl.when(usable(i) > 0)
        def _():
            for copy in copies(i):
                copy.start()

    def one(i, _):
        attend_one(
            scaling,
            info[2],
            usable(i),
            copies(i),
            q_buf.at[i],
            k_buf.at[i],
            v_buf.at[i],
            mine_ref.at[i],
            theirs_ref.at[i],
            s_ref,
            acc_ref,
        )
        return _

    lax.fori_loop(0, steps, one, 0)


def attend_one(scaling, core, usable, copies, q_ref, k_ref, v_ref, mine_ref, theirs_ref, s_ref, acc_ref):
    rows, head_dim = k_ref.shape
    queries = q_ref.shape[1]
    per_page = 2 * page
    pages = usable // page
    some = pages > 0
    factor = scaling * math.log2(math.e)
    d2 = 2 * head_dim

    even_row = lax.broadcasted_iota(jnp.int32, (16, head_dim), 0) % 2 == 0
    pick_even = jnp.where(even_row, 1.0, 0.0).astype(bf16)
    pick_odd = jnp.where(even_row, 0.0, 1.0).astype(bf16)

    @pl.when(some)
    def _():
        copies[0].wait()
        copies[1].wait()

    qc = jnp.concatenate([q_ref[0].T, q_ref[1].T], axis=0)

    def scores(p, tile):
        k = k_ref[pl.ds(p * per_page, tile), :].reshape(tile // 16, 16, head_dim)
        wide = jnp.concatenate(
            [
                (k * pick_even[None]).reshape(tile, head_dim),
                (k * pick_odd[None]).reshape(tile, head_dim),
            ],
            axis=1,
        )
        s = contract(wide, qc, 1, 0)
        s_ref[pl.ds(p * per_page, tile), :] = s
        return jnp.max(s.reshape(tile // 8, 8, queries), axis=0)

    def tops(most):
        even = lax.broadcasted_iota(jnp.int32, (8, queries), 0) % 2 == 0
        low = jnp.full_like(most, -jnp.inf)
        top0 = jnp.max(jnp.where(even, most, low), axis=0, keepdims=True)
        top1 = jnp.max(jnp.where(even, low, most), axis=0, keepdims=True)
        return top0, top1, jnp.where(even, top0, top1)

    def weighted(p, tile, both):
        s = s_ref[pl.ds(p * per_page, tile), :].reshape(tile // 8, 8, queries)
        w = jnp.exp2((s - both[None]) * factor).reshape(tile, queries).astype(bf16)
        v = v_ref[pl.ds(p * per_page, tile), :].T
        even = lax.broadcasted_iota(jnp.int32, (16, tile), 1) % 2 == 0
        even_lane = jnp.where(even, 1.0, 0.0).astype(bf16)
        odd_lane = jnp.where(even, 0.0, 1.0).astype(bf16)
        first = lax.broadcasted_iota(jnp.int32, (16, tile), 0)
        ones = jnp.where(
            first == 0, even_lane.astype(f32), jnp.where(first == 1, odd_lane.astype(f32), 0.0)
        ).astype(bf16)
        v3 = v.reshape(head_dim // 16, 16, tile)
        wide = jnp.concatenate(
            [
                (v3 * even_lane[None]).reshape(head_dim, tile),
                (v3 * odd_lane[None]).reshape(head_dim, tile),
                ones,
            ],
            axis=0,
        )
        return contract(wide, w, 1, 0)

    whole = rows // per_page
    spans, start = [], jnp.int32(0)
    for run in (whole, whole // 2, 1):
        count = (pages - start) // run
        spans.append((run, start, count))
        start = start + count * run

    def look(p, count, most):
        for i in range(count):
            most = jnp.maximum(most, scores(p + i, per_page))
        return most

    most = jnp.full((8, queries), -jnp.inf, f32)
    for run, start, count in spans:
        most = lax.fori_loop(
            0, count, lambda i, m, run=run, start=start: look(start + i * run, run, m), most
        )
    top0, top1, both = tops(most)
    acc_ref[...] = jnp.zeros_like(acc_ref)

    @pl.when(some)
    def _():
        copies[2].wait()

    def add(p, count):
        acc_ref[...] += sum(weighted(p + i, per_page, both) for i in range(count))

    for run, start, count in spans:
        lax.fori_loop(
            0, count, lambda i, _, run=run, start=start: add(start + i * run, run), None
        )
    a0, a1 = acc_ref[:head_dim], acc_ref[head_dim:d2]
    s0 = stats(jnp.where(some, top0 * scaling, very_low), acc_ref[d2 : d2 + 1])
    s1 = stats(jnp.where(some, top1 * scaling, very_low), acc_ref[d2 + 1 : d2 + 2])
    first = core == 0
    mine_ref[:head_dim, :] = jnp.where(first, a0, a1)
    theirs_ref[:head_dim, :] = jnp.where(first, a1, a0)
    mine_ref[head_dim:, :] = jnp.where(first, s0, s1)
    theirs_ref[head_dim:, :] = jnp.where(first, s1, s0)


def attend(query, key_cache, value_cache, info, scaling, order, steps):
    _, heads, queries, head_dim = query.shape
    rows = key_cache.shape[1]
    out = jax.ShapeDtypeStruct((steps, head_dim + stat_rows, queries), f32)
    cost = pl.CostEstimate(
        flops=8 * steps * rows * queries * head_dim,
        transcendentals=steps * rows * queries,
        bytes_accessed=4 * steps * rows * head_dim,
    )
    in_hbm = [pltpu.with_memory_space_constraint(x, pltpu.HBM) for x in (query, key_cache, value_cache)]
    return pl.pallas_call(
        functools.partial(attend_kernel, scaling, order),
        in_specs=[smem] + [pl.BlockSpec(memory_space=pltpu.HBM)] * 3,
        out_specs=[pl.BlockSpec(memory_space=VMEM)] * 2,
        out_shape=[out, out],
        scratch_shapes=[
            VMEM((steps, heads, queries, head_dim), bf16),
            VMEM((steps, rows, head_dim), bf16),
            VMEM((steps, rows, head_dim), bf16),
            VMEM((rows, queries), f32),
            VMEM((2 * head_dim + 16, queries), f32),
            pltpu.SemaphoreType.DMA((steps, 3)),
        ],
        name="attend",
        compiler_params=limit(24),
        cost_estimate=cost,
    )(info, *in_hbm)


def merged(parts, depth):
    tops = [p[depth : depth + 1] for p in parts]
    top = functools.reduce(jnp.maximum, tops)
    shares = [jnp.exp(t - top) for t in tops]
    numer = sum(p[:depth] * e for p, e in zip(parts, shares))
    total = sum(p[depth + 1 : depth + 2] * e for p, e in zip(parts, shares))
    return numer, top, total


def merge_core_kernel(mine_ref, got_ref, *outs):
    depth = mine_ref.shape[1] - stat_rows
    for k, out in enumerate(outs):
        numer, top, total = merged([mine_ref[k], got_ref[k]], depth)
        out[:depth, :] = numer
        out[depth:, :] = stats(top, total)


def merge_kernel(*refs):
    parts, out = refs[:-1], refs[-1]
    depth = out.shape[0] - stat_rows
    numer, top, total = merged([p[...] for p in parts], depth)
    out[:depth, :] = numer
    out[depth:, :] = stats(top, total)


def finish_kernel(scaling, draft, info, *refs):
    parts, (q_ref, key_ref, value_ref), out = refs[:-4], refs[-4:-1], refs[-1]
    depth = parts[0].shape[0] - stat_rows
    numer, top, total = merged([p[...] for p in parts], depth)
    own = contract(key_ref[info[1], info[2]], q_ref[info[1], info[2]], 1, 1) * scaling
    at = lax.broadcasted_iota(jnp.int32, own.shape, 0)
    row = lax.broadcasted_iota(jnp.int32, own.shape, 1) % draft
    causal = at <= row
    own = jnp.where(causal, own, very_low)
    overall = jnp.maximum(top, jnp.max(own, axis=0, keepdims=True))
    carried = jnp.exp(top - overall)
    fresh = jnp.where(causal, jnp.exp(own - overall), 0.0)
    denominator = total * carried + jnp.sum(fresh, axis=0, keepdims=True)
    added = contract(value_ref[info[1], info[2]].astype(f32), fresh, 0, 0, lax.Precision.HIGHEST)
    out[...] = ((numer * carried + added) / denominator).astype(bf16).astype(f32)


def project_kernel(draft, info, *refs):
    pieces, (w_ref, out_ref, x_ref) = refs[:-3], refs[-3:]
    width = x_ref.shape[2]
    for i, piece in enumerate(pieces):
        k, other = i // 2, i % 2
        g = jnp.bitwise_xor(info[2], other)
        seq = jnp.bitwise_xor(info[1], k)
        at = pl.ds(pl.multiple_of(seq * draft, draft), draft)
        depth, queries = piece.shape
        for a in range(queries // depth):
            att = piece[:, a * depth : (a + 1) * depth].T.astype(bf16)
            for h in range(depth // draft):
                col = (a * (depth // draft) + h) * depth
                x_ref[g, at, col : col + depth] = att[h * draft : (h + 1) * draft]
    out_ref[...] = sum(contract(x_ref[g], w_ref[g * width : (g + 1) * width, :], 1, 0) for g in range(2))


def whole_vmem(n):
    return [pl.BlockSpec(memory_space=VMEM)] * n


def limit(mib):
    return pltpu.CompilerParams(vmem_limit_bytes=mib * 2**20)


smem = pl.BlockSpec(memory_space=pltpu.SMEM)


def step(query, key_cache, value_cache, new_key, new_value, lengths, out_weight):
    seqs, q_count, draft, head_dim = query.shape
    ctx_len, heads = key_cache.shape[1], key_cache.shape[2]
    queries = q_count // heads * draft
    scaling = 1.0 / math.sqrt(head_dim)
    n_ctx = lax.axis_size("ctx")
    chips = n_ctx // 2
    far = chips // radix

    def place(z, c):
        return (z - c * (radix // 2)) % chips // radix, z % radix

    def chip(b, j, c):
        shift = c * (radix // 2)
        return (b * radix + shift + (j - shift) % radix) % chips

    def pairs(k):
        out = []
        for i in range(n_ctx):
            z, c = divmod(i, 2)
            b, j = place(z, c)
            out.append((i, 2 * chip(b, j ^ k, c) + c))
        return out

    def partner(i, n, turn):
        return i ^ 1 if turn == 0 else (((i + 1) % n) ^ 1) - 1 if ((i + 1) % n) ^ 1 else n - 1

    near_pairs = [pairs(k) for k in range(radix)]
    far_pairs = [
        [
            (i, 2 * (partner(z // radix, far, t ^ c) * radix + z % radix) + c)
            for i in range(n_ctx)
            for z, c in [divmod(i, 2)]
        ]
        for t in range(2)
    ]
    n_head = lax.axis_size("head")
    head_pairs = [
        [
            (i * n_head + h, i * n_head + partner(h, n_head, t ^ (i % 2)))
            for i in range(n_ctx)
            for h in range(n_head)
        ]
        for t in range(2)
    ]
    core_pairs = [(i, i ^ 1) for i in range(n_ctx)]

    swap = lambda x: lax.ppermute(x, "ctx", core_pairs)
    to_near = lambda x, k: lax.ppermute(x, "ctx", near_pairs[k])
    to_far = lambda x, t: lax.ppermute(x, "ctx", far_pairs[t])
    to_head = lambda x, t: lax.ppermute(x, ("ctx", "head"), head_pairs[t])

    index = lax.axis_index("ctx")
    core = index % 2
    spot = place(index // 2, core)[1]
    info = jnp.concatenate([jnp.stack([index * ctx_len, spot, core]).astype(jnp.int32), lengths])

    grouped = query.reshape(seqs, heads, queries, head_dim)
    keys = key_cache.reshape(seqs, ctx_len * heads, head_dim)
    values = value_cache.reshape(seqs, ctx_len * heads, head_dim)
    chunk = jax.ShapeDtypeStruct((head_dim + stat_rows, queries), f32)
    half_seqs = seqs // 2
    gate = info
    chunks = {}
    for half in range(2):
        order = lambda k, half=half: seqs - 1 - half * half_seqs - k
        mine, theirs = attend(grouped, keys, values, gate, scaling, order, half_seqs)
        got = swap(theirs)
        found = pl.pallas_call(
            merge_core_kernel,
            in_specs=whole_vmem(2),
            out_specs=whole_vmem(half_seqs),
            out_shape=[chunk] * half_seqs,
            name="merge_core",
            compiler_params=limit(8),
        )(mine, got)
        gate, *found = lax.optimization_barrier((info, *found))
        for k, x in enumerate(found):
            chunks[order(k)] = to_near(x, order(k)) if order(k) else x
    chunks = [chunks[k] for k in range(radix)]

    def merge(parts):
        return pl.pallas_call(
            merge_kernel,
            in_specs=whole_vmem(len(parts)),
            out_specs=pl.BlockSpec(memory_space=VMEM),
            out_shape=chunk,
            name="merge",
            compiler_params=limit(4),
        )(*parts)

    found = merge(chunks)
    found = merge([found, to_far(found, 0)])
    parts = [found, to_far(found, 1)]
    att = pl.pallas_call(
        functools.partial(finish_kernel, scaling, draft),
        in_specs=[smem] + whole_vmem(5),
        out_specs=pl.BlockSpec(memory_space=VMEM),
        out_shape=jax.ShapeDtypeStruct((head_dim, queries), f32),
        name="finish",
        compiler_params=limit(4),
    )(info, *parts, grouped, new_key, new_value)
    near = [att] + [to_near(att, k) for k in range(1, radix)]
    pieces = []
    for part in near:
        pieces += [part, swap(part)]
    width = out_weight.shape[1]
    out = pl.pallas_call(
        functools.partial(project_kernel, draft),
        in_specs=[smem] + whole_vmem(len(pieces) + 1),
        out_specs=pl.BlockSpec(memory_space=VMEM),
        out_shape=jax.ShapeDtypeStruct((seqs * draft, width), f32),
        scratch_shapes=[VMEM((heads, seqs * draft, out_weight.shape[0] // heads), bf16)],
        name="project",
        compiler_params=limit(8),
    )(info, *pieces, out_weight)
    for t in range(2):
        out = out + to_head(out, t)
    return out.reshape(seqs, draft, width)


def solution(mesh):
    placed = (
        P("groups", "head", None, None),
        P("groups", "ctx", "head", None),
        P("groups", "ctx", "head", None),
        P("groups", "head", None, None),
        P("groups", "head", None, None),
        P("groups"),
        P("head", "ctx"),
    )
    return jax.shard_map(
        step, mesh=mesh, in_specs=placed, out_specs=P("groups", None, "ctx"), check_vma=False
    )
```

```python
import functools
import math

import jax
import jax.numpy as jnp
from jax import lax
from jax.experimental import pallas as pl
from jax.experimental.pallas import tpu as pltpu
from jax.sharding import PartitionSpec as P


very_low = -1e30
page = 256
radix = 4
stat_rows = 8

VMEM = pltpu.VMEM
f32 = jnp.float32
bf16 = jnp.bfloat16


def stats(top, total):
    row = lax.broadcasted_iota(jnp.int32, (stat_rows, top.shape[-1]), 0)
    return jnp.where(row == 0, top, jnp.where(row == 1, total, 0.0))


def contract(a, b, da, db, precision=None):
    return lax.dot_general(
        a, b, (((da,), (db,)), ((), ())), preferred_element_type=f32, precision=precision
    )


def attend_kernel(scaling, order, info, q_hbm, k_hbm, v_hbm, mine_ref, theirs_ref, *scratch):
    q_buf, k_buf, v_buf, s_ref, acc_ref, sems = scratch
    steps = q_buf.shape[0]

    def copies(i):
        seq = lax.rem(info[1] + order(i), radix)
        return [
            pltpu.make_async_copy(hbm.at[seq], buf.at[i], sems.at[i, n])
            for n, (hbm, buf) in enumerate(((q_hbm, q_buf), (k_hbm, k_buf), (v_hbm, v_buf)))
        ]

    def usable(i):
        seq = lax.rem(info[1] + order(i), radix)
        return jnp.clip(info[3 + seq] - info[0], 0, k_buf.shape[1] // 2)

    for i in range(steps):

        @pl.when(usable(i) > 0)
        def _():
            for copy in copies(i):
                copy.start()

    def one(i, _):
        attend_one(
            scaling,
            info[2],
            usable(i),
            copies(i),
            q_buf.at[i],
            k_buf.at[i],
            v_buf.at[i],
            mine_ref.at[i],
            theirs_ref.at[i],
            s_ref,
            acc_ref,
        )
        return _

    lax.fori_loop(0, steps, one, 0)


def attend_one(scaling, core, usable, copies, q_ref, k_ref, v_ref, mine_ref, theirs_ref, s_ref, acc_ref):
    rows, head_dim = k_ref.shape
    queries = q_ref.shape[1]
    per_page = 2 * page
    pages = usable // page
    some = pages > 0
    factor = scaling * math.log2(math.e)
    d2 = 2 * head_dim

    even_row = lax.broadcasted_iota(jnp.int32, (16, head_dim), 0) % 2 == 0
    pick_even = jnp.where(even_row, 1.0, 0.0).astype(bf16)
    pick_odd = jnp.where(even_row, 0.0, 1.0).astype(bf16)

    @pl.when(some)
    def _():
        copies[0].wait()
        copies[1].wait()

    qc = jnp.concatenate([q_ref[0].T, q_ref[1].T], axis=0)

    def scores(p, tile):
        k = k_ref[pl.ds(p * per_page, tile), :].reshape(tile // 16, 16, head_dim)
        wide = jnp.concatenate(
            [
                (k * pick_even[None]).reshape(tile, head_dim),
                (k * pick_odd[None]).reshape(tile, head_dim),
            ],
            axis=1,
        )
        s = contract(wide, qc, 1, 0)
        s_ref[pl.ds(p * per_page, tile), :] = s
        return jnp.max(s.reshape(tile // 8, 8, queries), axis=0)

    def tops(most):
        even = lax.broadcasted_iota(jnp.int32, (8, queries), 0) % 2 == 0
        low = jnp.full_like(most, -jnp.inf)
        top0 = jnp.max(jnp.where(even, most, low), axis=0, keepdims=True)
        top1 = jnp.max(jnp.where(even, low, most), axis=0, keepdims=True)
        return top0, top1, jnp.where(even, top0, top1)

    def weighted(p, tile, both):
        s = s_ref[pl.ds(p * per_page, tile), :].reshape(tile // 8, 8, queries)
        w = jnp.exp2((s - both[None]) * factor).reshape(tile, queries).astype(bf16)
        v = v_ref[pl.ds(p * per_page, tile), :].T
        even = lax.broadcasted_iota(jnp.int32, (16, tile), 1) % 2 == 0
        even_lane = jnp.where(even, 1.0, 0.0).astype(bf16)
        odd_lane = jnp.where(even, 0.0, 1.0).astype(bf16)
        first = lax.broadcasted_iota(jnp.int32, (16, tile), 0)
        ones = jnp.where(
            first == 0, even_lane.astype(f32), jnp.where(first == 1, odd_lane.astype(f32), 0.0)
        ).astype(bf16)
        v3 = v.reshape(head_dim // 16, 16, tile)
        wide = jnp.concatenate(
            [
                (v3 * even_lane[None]).reshape(head_dim, tile),
                (v3 * odd_lane[None]).reshape(head_dim, tile),
                ones,
            ],
            axis=0,
        )
        return contract(wide, w, 1, 0)

    whole = rows // per_page
    spans, start = [], jnp.int32(0)
    for run in (whole, whole // 2, 1):
        count = (pages - start) // run
        spans.append((run, start, count))
        start = start + count * run

    def look(p, count, most):
        for i in range(count):
            most = jnp.maximum(most, scores(p + i, per_page))
        return most

    most = jnp.full((8, queries), -jnp.inf, f32)
    for run, start, count in spans:
        most = lax.fori_loop(
            0, count, lambda i, m, run=run, start=start: look(start + i * run, run, m), most
        )
    top0, top1, both = tops(most)
    acc_ref[...] = jnp.zeros_like(acc_ref)

    @pl.when(some)
    def _():
        copies[2].wait()

    def add(p, count):
        acc_ref[...] += sum(weighted(p + i, per_page, both) for i in range(count))

    for run, start, count in spans:
        lax.fori_loop(
            0, count, lambda i, _, run=run, start=start: add(start + i * run, run), None
        )
    a0, a1 = acc_ref[:head_dim], acc_ref[head_dim:d2]
    s0 = stats(jnp.where(some, top0 * scaling, very_low), acc_ref[d2 : d2 + 1])
    s1 = stats(jnp.where(some, top1 * scaling, very_low), acc_ref[d2 + 1 : d2 + 2])
    first = core == 0
    mine_ref[:head_dim, :] = jnp.where(first, a0, a1)
    theirs_ref[:head_dim, :] = jnp.where(first, a1, a0)
    mine_ref[head_dim:, :] = jnp.where(first, s0, s1)
    theirs_ref[head_dim:, :] = jnp.where(first, s1, s0)


def attend(query, key_cache, value_cache, info, scaling, order, steps):
    _, heads, queries, head_dim = query.shape
    rows = key_cache.shape[1]
    out = jax.ShapeDtypeStruct((steps, head_dim + stat_rows, queries), f32)
    cost = pl.CostEstimate(
        flops=8 * steps * rows * queries * head_dim,
        transcendentals=steps * rows * queries,
        bytes_accessed=4 * steps * rows * head_dim,
    )
    in_hbm = [pltpu.with_memory_space_constraint(x, pltpu.HBM) for x in (query, key_cache, value_cache)]
    return pl.pallas_call(
        functools.partial(attend_kernel, scaling, order),
        in_specs=[smem] + [pl.BlockSpec(memory_space=pltpu.HBM)] * 3,
        out_specs=[pl.BlockSpec(memory_space=VMEM)] * 2,
        out_shape=[out, out],
        scratch_shapes=[
            VMEM((steps, heads, queries, head_dim), bf16),
            VMEM((steps, rows, head_dim), bf16),
            VMEM((steps, rows, head_dim), bf16),
            VMEM((rows, queries), f32),
            VMEM((2 * head_dim + 16, queries), f32),
            pltpu.SemaphoreType.DMA((steps, 3)),
        ],
        name="attend",
        compiler_params=limit(24),
        cost_estimate=cost,
    )(info, *in_hbm)


def merged(parts, depth):
    tops = [p[depth : depth + 1] for p in parts]
    top = functools.reduce(jnp.maximum, tops)
    shares = [jnp.exp(t - top) for t in tops]
    numer = sum(p[:depth] * e for p, e in zip(parts, shares))
    total = sum(p[depth + 1 : depth + 2] * e for p, e in zip(parts, shares))
    return numer, top, total


def merge_core_kernel(mine_ref, got_ref, *outs):
    depth = mine_ref.shape[1] - stat_rows
    for k, out in enumerate(outs):
        numer, top, total = merged([mine_ref[k], got_ref[k]], depth)
        out[:depth, :] = numer
        out[depth:, :] = stats(top, total)


def merge_kernel(*refs):
    parts, out = refs[:-1], refs[-1]
    depth = out.shape[0] - stat_rows
    numer, top, total = merged([p[...] for p in parts], depth)
    out[:depth, :] = numer
    out[depth:, :] = stats(top, total)


def own_kernel(scaling, draft, info, q_ref, key_ref, value_ref, out):
    depth = out.shape[0] - stat_rows
    own = contract(key_ref[info[1], info[2]], q_ref[info[1], info[2]], 1, 1) * scaling
    at = lax.broadcasted_iota(jnp.int32, own.shape, 0)
    row = lax.broadcasted_iota(jnp.int32, own.shape, 1) % draft
    causal = at <= row
    own = jnp.where(causal, own, very_low)
    top = jnp.max(own, axis=0, keepdims=True)
    fresh = jnp.where(causal, jnp.exp(own - top), 0.0)
    values = value_ref[info[1], info[2]].astype(f32)
    out[:depth, :] = contract(values, fresh, 0, 0, lax.Precision.HIGHEST)
    out[depth:, :] = stats(top, jnp.sum(fresh, axis=0, keepdims=True))


def finish_kernel(*refs):
    parts, out = refs[:-1], refs[-1]
    numer, _, total = merged([p[...] for p in parts], out.shape[0])
    out[...] = (numer / total).astype(bf16).astype(f32)


def project_kernel(draft, info, *refs):
    pieces, (w_ref, out_ref, x_ref) = refs[:-3], refs[-3:]
    width = x_ref.shape[2]
    for i, piece in enumerate(pieces):
        k, other = i // 2, i % 2
        g = jnp.bitwise_xor(info[2], other)
        seq = lax.rem(info[1] + k, radix)
        at = pl.ds(pl.multiple_of(seq * draft, draft), draft)
        depth, queries = piece.shape
        for a in range(queries // depth):
            att = piece[:, a * depth : (a + 1) * depth].T.astype(bf16)
            for h in range(depth // draft):
                col = (a * (depth // draft) + h) * depth
                x_ref[g, at, col : col + depth] = att[h * draft : (h + 1) * draft]
    out_ref[...] = sum(contract(x_ref[g], w_ref[g * width : (g + 1) * width, :], 1, 0) for g in range(2))


def whole_vmem(n):
    return [pl.BlockSpec(memory_space=VMEM)] * n


def limit(mib):
    return pltpu.CompilerParams(vmem_limit_bytes=mib * 2**20)


smem = pl.BlockSpec(memory_space=pltpu.SMEM)


def step(query, key_cache, value_cache, new_key, new_value, lengths, out_weight):
    seqs, q_count, draft, head_dim = query.shape
    ctx_len, heads = key_cache.shape[1], key_cache.shape[2]
    queries = q_count // heads * draft
    scaling = 1.0 / math.sqrt(head_dim)
    n_ctx = lax.axis_size("ctx")
    chips = n_ctx // 2
    far = chips // radix

    def near_to(k):
        out = []
        for i in range(n_ctx):
            z, c = divmod(i, 2)
            step = {0: 0, 1: 1, 2: 2 - 4 * c, 3: -1}[k]
            out.append((i, 2 * ((z + step) % chips) + c))
        return out

    def partner(i, n, turn):
        return i ^ 1 if turn == 0 else (((i + 1) % n) ^ 1) - 1 if ((i + 1) % n) ^ 1 else n - 1

    near_pairs = [near_to(k) for k in range(radix)]
    far_pairs = [
        [
            (i, 2 * (partner(z // radix, far, t ^ c) * radix + z % radix) + c)
            for i in range(n_ctx)
            for z, c in [divmod(i, 2)]
        ]
        for t in range(2)
    ]
    n_head = lax.axis_size("head")
    head_pairs = [
        [
            (i * n_head + h, i * n_head + partner(h, n_head, t ^ (i % 2)))
            for i in range(n_ctx)
            for h in range(n_head)
        ]
        for t in range(2)
    ]
    core_pairs = [(i, i ^ 1) for i in range(n_ctx)]

    swap = lambda x: lax.ppermute(x, "ctx", core_pairs)
    to_near = lambda x, k: lax.ppermute(x, "ctx", near_pairs[k])
    to_far = lambda x, t: lax.ppermute(x, "ctx", far_pairs[t])
    to_head = lambda x, t: lax.ppermute(x, ("ctx", "head"), head_pairs[t])

    index = lax.axis_index("ctx")
    core = index % 2
    spot = index // 2 % radix
    info = jnp.concatenate([jnp.stack([index * ctx_len, spot, core]).astype(jnp.int32), lengths])

    grouped = query.reshape(seqs, heads, queries, head_dim)
    keys = key_cache.reshape(seqs, ctx_len * heads, head_dim)
    values = value_cache.reshape(seqs, ctx_len * heads, head_dim)
    chunk = jax.ShapeDtypeStruct((head_dim + stat_rows, queries), f32)
    gate = info
    chunks = {}
    for steps in ((2, 1, 3), (0,)):
        order = lambda i, steps=steps: functools.reduce(
            lambda at, n: jnp.where(i == n, steps[n], at), range(1, len(steps)), jnp.int32(steps[0])
        )
        mine, theirs = attend(grouped, keys, values, gate, scaling, order, len(steps))
        got = swap(theirs)
        found = pl.pallas_call(
            merge_core_kernel,
            in_specs=whole_vmem(2),
            out_specs=whole_vmem(len(steps)),
            out_shape=[chunk] * len(steps),
            name="merge_core",
            compiler_params=limit(8),
        )(mine, got)
        gate, *found = lax.optimization_barrier((info, *found))
        for k, x in zip(steps, found):
            chunks[k] = to_near(x, k) if k else x
    chunks = [chunks[k] for k in range(radix)]

    def merge(parts):
        return pl.pallas_call(
            merge_kernel,
            in_specs=whole_vmem(len(parts)),
            out_specs=pl.BlockSpec(memory_space=VMEM),
            out_shape=chunk,
            name="merge",
            compiler_params=limit(4),
        )(*parts)

    found = merge(chunks)
    found = merge([found, to_far(found, 0)])
    own = pl.pallas_call(
        functools.partial(own_kernel, scaling, draft),
        in_specs=[smem] + whole_vmem(3),
        out_specs=pl.BlockSpec(memory_space=VMEM),
        out_shape=chunk,
        name="own",
        compiler_params=limit(4),
    )(info, grouped, new_key, new_value)
    parts = [found, to_far(found, 1), own]
    att = pl.pallas_call(
        finish_kernel,
        in_specs=whole_vmem(len(parts)),
        out_specs=pl.BlockSpec(memory_space=VMEM),
        out_shape=jax.ShapeDtypeStruct((head_dim, queries), f32),
        name="finish",
        compiler_params=limit(4),
    )(*parts)
    near = [att] + [to_near(att, radix - k) for k in range(1, radix)]
    pieces = []
    for part in near:
        pieces += [part, swap(part)]
    width = out_weight.shape[1]
    out = pl.pallas_call(
        functools.partial(project_kernel, draft),
        in_specs=[smem] + whole_vmem(len(pieces) + 1),
        out_specs=pl.BlockSpec(memory_space=VMEM),
        out_shape=jax.ShapeDtypeStruct((seqs * draft, width), f32),
        scratch_shapes=[VMEM((heads, seqs * draft, out_weight.shape[0] // heads), bf16)],
        name="project",
        compiler_params=limit(8),
    )(info, *pieces, out_weight)
    for t in range(2):
        out = out + to_head(out, t)
    return out.reshape(seqs, draft, width)


def solution(mesh):
    placed = (
        P("groups", "head", None, None),
        P("groups", "ctx", "head", None),
        P("groups", "ctx", "head", None),
        P("groups", "head", None, None),
        P("groups", "head", None, None),
        P("groups"),
        P("head", "ctx"),
    )
    return jax.shard_map(
        step, mesh=mesh, in_specs=placed, out_specs=P("groups", None, "ctx"), check_vma=False
    )
```

```python
import functools
import math

import jax
import jax.numpy as jnp
from jax import lax
from jax.experimental import pallas as pl
from jax.experimental.pallas import tpu as pltpu
from jax.sharding import PartitionSpec as P


very_low = -1e30
page = 256
radix = 4
stat_rows = 8

VMEM = pltpu.VMEM
f32 = jnp.float32
bf16 = jnp.bfloat16


def stats(top, total):
    row = lax.broadcasted_iota(jnp.int32, (stat_rows, top.shape[-1]), 0)
    return jnp.where(row == 0, top, jnp.where(row == 1, total, 0.0))


def contract(a, b, da, db, precision=None):
    return lax.dot_general(
        a, b, (((da,), (db,)), ((), ())), preferred_element_type=f32, precision=precision
    )


def attend_kernel(scaling, order, ahead, info, q_hbm, k_hbm, v_hbm, *refs):
    n_out = 2 + 3 * ahead
    mine_ref, theirs_ref, *next_refs = refs[:n_out]
    q_buf, k_buf, v_buf, s_ref, acc_ref, sems = refs[n_out:]
    steps = q_buf.shape[0]

    def usable(seq):
        return jnp.clip(info[3 + seq] - info[0], 0, k_buf.shape[1] // 2)

    def seq_of(i):
        return lax.rem(info[1] + order(i), radix)

    def copies(i, seq, bufs):
        return [
            pltpu.make_async_copy(hbm.at[seq], buf, sems.at[i, n])
            for n, (hbm, buf) in enumerate(zip((q_hbm, k_hbm, v_hbm), bufs))
        ]

    def slot(i):
        return copies(i, seq_of(i), (q_buf.at[i], k_buf.at[i], v_buf.at[i]))

    for i in range(steps):

        @pl.when(usable(seq_of(i)) > 0)
        def _():
            for copy in slot(i):
                copy.start()

    if ahead:
        later = copies(steps, info[1], next_refs)

        @pl.when(usable(info[1]) > 0)
        def _():
            for copy in later:
                copy.start()

    def one(i, _):
        count = usable(seq_of(i))
        refs = (q_buf.at[i], k_buf.at[i], v_buf.at[i], mine_ref.at[i], theirs_ref.at[i])
        attend_one(scaling, info[2], count, slot(i), *refs, s_ref, acc_ref)
        return _

    lax.fori_loop(0, steps, one, 0)
    if ahead:

        @pl.when(usable(info[1]) > 0)
        def _():
            for copy in later:
                copy.wait()


def attend_last_kernel(scaling, info, q_ref, k_ref, v_ref, mine_ref, theirs_ref, s_ref, acc_ref):
    count = jnp.clip(info[3 + info[1]] - info[0], 0, k_ref.shape[0] // 2)
    refs = (q_ref, k_ref, v_ref, mine_ref.at[0], theirs_ref.at[0])
    attend_one(scaling, info[2], count, None, *refs, s_ref, acc_ref)


def attend_one(scaling, core, usable, copies, q_ref, k_ref, v_ref, mine_ref, theirs_ref, s_ref, acc_ref):
    rows, head_dim = k_ref.shape
    queries = q_ref.shape[1]
    per_page = 2 * page
    pages = usable // page
    some = pages > 0
    factor = scaling * math.log2(math.e)
    d2 = 2 * head_dim

    even_row = lax.broadcasted_iota(jnp.int32, (16, head_dim), 0) % 2 == 0
    pick_even = jnp.where(even_row, 1.0, 0.0).astype(bf16)
    pick_odd = jnp.where(even_row, 0.0, 1.0).astype(bf16)

    if copies:

        @pl.when(some)
        def _():
            copies[0].wait()
            copies[1].wait()

    qc = jnp.concatenate([q_ref[0].T, q_ref[1].T], axis=0)

    def scores(p, tile):
        k = k_ref[pl.ds(p * per_page, tile), :].reshape(tile // 16, 16, head_dim)
        wide = jnp.concatenate(
            [
                (k * pick_even[None]).reshape(tile, head_dim),
                (k * pick_odd[None]).reshape(tile, head_dim),
            ],
            axis=1,
        )
        s = contract(wide, qc, 1, 0)
        s_ref[pl.ds(p * per_page, tile), :] = s
        return jnp.max(s.reshape(tile // 8, 8, queries), axis=0)

    def tops(most):
        even = lax.broadcasted_iota(jnp.int32, (8, queries), 0) % 2 == 0
        low = jnp.full_like(most, -jnp.inf)
        top0 = jnp.max(jnp.where(even, most, low), axis=0, keepdims=True)
        top1 = jnp.max(jnp.where(even, low, most), axis=0, keepdims=True)
        return top0, top1, jnp.where(even, top0, top1)

    def weighted(p, tile, both):
        s = s_ref[pl.ds(p * per_page, tile), :].reshape(tile // 8, 8, queries)
        w = jnp.exp2((s - both[None]) * factor).reshape(tile, queries).astype(bf16)
        v = v_ref[pl.ds(p * per_page, tile), :].T
        even = lax.broadcasted_iota(jnp.int32, (16, tile), 1) % 2 == 0
        even_lane = jnp.where(even, 1.0, 0.0).astype(bf16)
        odd_lane = jnp.where(even, 0.0, 1.0).astype(bf16)
        first = lax.broadcasted_iota(jnp.int32, (16, tile), 0)
        ones = jnp.where(
            first == 0, even_lane.astype(f32), jnp.where(first == 1, odd_lane.astype(f32), 0.0)
        ).astype(bf16)
        v3 = v.reshape(head_dim // 16, 16, tile)
        wide = jnp.concatenate(
            [
                (v3 * even_lane[None]).reshape(head_dim, tile),
                (v3 * odd_lane[None]).reshape(head_dim, tile),
                ones,
            ],
            axis=0,
        )
        return contract(wide, w, 1, 0)

    whole = rows // per_page
    spans, start = [], jnp.int32(0)
    for run in (whole, whole // 2, 1):
        count = (pages - start) // run
        spans.append((run, start, count))
        start = start + count * run

    def look(p, count, most):
        for i in range(count):
            most = jnp.maximum(most, scores(p + i, per_page))
        return most

    most = jnp.full((8, queries), -jnp.inf, f32)
    for run, start, count in spans:
        most = lax.fori_loop(
            0, count, lambda i, m, run=run, start=start: look(start + i * run, run, m), most
        )
    top0, top1, both = tops(most)
    acc_ref[...] = jnp.zeros_like(acc_ref)

    if copies:

        @pl.when(some)
        def _():
            copies[2].wait()

    def add(p, count):
        acc_ref[...] += sum(weighted(p + i, per_page, both) for i in range(count))

    for run, start, count in spans:
        lax.fori_loop(
            0, count, lambda i, _, run=run, start=start: add(start + i * run, run), None
        )
    a0, a1 = acc_ref[:head_dim], acc_ref[head_dim:d2]
    s0 = stats(jnp.where(some, top0 * scaling, very_low), acc_ref[d2 : d2 + 1])
    s1 = stats(jnp.where(some, top1 * scaling, very_low), acc_ref[d2 + 1 : d2 + 2])
    first = core == 0
    mine_ref[:head_dim, :] = jnp.where(first, a0, a1)
    theirs_ref[:head_dim, :] = jnp.where(first, a1, a0)
    mine_ref[head_dim:, :] = jnp.where(first, s0, s1)
    theirs_ref[head_dim:, :] = jnp.where(first, s1, s0)


def attend(query, key_cache, value_cache, info, scaling, steps):
    _, heads, queries, head_dim = query.shape
    rows = key_cache.shape[1]
    block = (head_dim + stat_rows, queries)
    work = [VMEM((rows, queries), f32), VMEM((2 * head_dim + 16, queries), f32)]

    def cost(n):
        return pl.CostEstimate(
            flops=8 * n * rows * queries * head_dim,
            transcendentals=n * rows * queries,
            bytes_accessed=4 * n * rows * head_dim,
        )

    def outs(n):
        return [jax.ShapeDtypeStruct((n, *block), f32)] * 2

    def order(i):
        at = jnp.int32(steps[0])
        for n, k in enumerate(steps):
            at = jnp.where(i == n, k, at)
        return at

    n = len(steps)
    in_hbm = [pltpu.with_memory_space_constraint(x, pltpu.HBM) for x in (query, key_cache, value_cache)]
    *most, q, k, v = pl.pallas_call(
        functools.partial(attend_kernel, scaling, order, True),
        in_specs=[smem] + [pl.BlockSpec(memory_space=pltpu.HBM)] * 3,
        out_specs=whole_vmem(5),
        out_shape=outs(n)
        + [jax.ShapeDtypeStruct(x.shape[1:], x.dtype) for x in (query, key_cache, value_cache)],
        scratch_shapes=[
            VMEM((n, heads, queries, head_dim), bf16),
            VMEM((n, rows, head_dim), bf16),
            VMEM((n, rows, head_dim), bf16),
            *work,
            pltpu.SemaphoreType.DMA((n + 1, 3)),
        ],
        name="attend",
        compiler_params=limit(26),
        cost_estimate=cost(n),
    )(info, *in_hbm)

    def last(info):
        return pl.pallas_call(
            functools.partial(attend_last_kernel, scaling),
            in_specs=[smem] + whole_vmem(3),
            out_specs=whole_vmem(2),
            out_shape=outs(1),
            scratch_shapes=work,
            name="attend_last",
            compiler_params=limit(16),
            cost_estimate=cost(1),
        )(info, q, k, v)

    return most, last


def merged(parts, depth):
    tops = [p[depth : depth + 1] for p in parts]
    top = functools.reduce(jnp.maximum, tops)
    shares = [jnp.exp(t - top) for t in tops]
    numer = sum(p[:depth] * e for p, e in zip(parts, shares))
    total = sum(p[depth + 1 : depth + 2] * e for p, e in zip(parts, shares))
    return numer, top, total


def merge_core_kernel(mine_ref, got_ref, *outs):
    depth = mine_ref.shape[1] - stat_rows
    for k, out in enumerate(outs):
        numer, top, total = merged([mine_ref[k], got_ref[k]], depth)
        out[:depth, :] = numer
        out[depth:, :] = stats(top, total)


def put_halves(outs, numer, top, total):
    depth, lanes = numer.shape[0], outs[0].shape[1]
    for n, out in enumerate(outs):
        at = slice(n * lanes, (n + 1) * lanes)
        out[:depth, :] = numer[:, at]
        out[depth:, :] = stats(top[:, at], total[:, at])


def merge_kernel(n_out, *refs):
    parts, outs = refs[:-n_out], refs[-n_out:]
    put_halves(outs, *merged([p[...] for p in parts], outs[0].shape[0] - stat_rows))


def own_kernel(scaling, draft, info, q_ref, key_ref, value_ref, *outs):
    own = contract(key_ref[info[1], info[2]], q_ref[info[1], info[2]], 1, 1) * scaling
    at = lax.broadcasted_iota(jnp.int32, own.shape, 0)
    row = lax.broadcasted_iota(jnp.int32, own.shape, 1) % draft
    causal = at <= row
    own = jnp.where(causal, own, very_low)
    top = jnp.max(own, axis=0, keepdims=True)
    fresh = jnp.where(causal, jnp.exp(own - top), 0.0)
    values = value_ref[info[1], info[2]].astype(f32)
    numer = contract(values, fresh, 0, 0, lax.Precision.HIGHEST)
    put_halves(outs, numer, top, jnp.sum(fresh, axis=0, keepdims=True))


def finish_kernel(*refs):
    parts, out = refs[:-1], refs[-1]
    numer, _, total = merged([p[...] for p in parts], out.shape[0])
    out[...] = (numer / total).astype(bf16).astype(f32)


def project_kernel(draft, half, info, *refs):
    n = 2 * radix
    pieces, extra, (w_ref, out_ref, x_ref) = refs[:n], refs[n:-3], refs[-3:]
    width = x_ref.shape[2]
    for i, piece in enumerate(pieces):
        k, other = i // 2, i % 2
        g = jnp.bitwise_xor(info[2], other)
        seq = lax.rem(info[1] + k, radix)
        at = pl.ds(pl.multiple_of(seq * draft, draft), draft)
        depth, lanes = piece.shape
        att = piece[...].T.astype(bf16)
        for h in range(lanes // draft):
            x_ref[g, at, h * depth : (h + 1) * depth] = att[h * draft : (h + 1) * draft]
    whole = w_ref.shape[0] // 2
    products = [
        contract(x_ref[g], w_ref[g * whole + half * width : g * whole + (half + 1) * width, :], 1, 0)
        for g in range(2)
    ]
    out_ref[...] = sum(products + [e[...] for e in extra])


def whole_vmem(n):
    return [pl.BlockSpec(memory_space=VMEM)] * n


def limit(mib):
    return pltpu.CompilerParams(vmem_limit_bytes=mib * 2**20)


smem = pl.BlockSpec(memory_space=pltpu.SMEM)


def step(query, key_cache, value_cache, new_key, new_value, lengths, out_weight):
    seqs, q_count, draft, head_dim = query.shape
    ctx_len, heads = key_cache.shape[1], key_cache.shape[2]
    queries = q_count // heads * draft
    scaling = 1.0 / math.sqrt(head_dim)
    n_ctx = lax.axis_size("ctx")
    chips = n_ctx // 2
    far = chips // radix

    def near_to(k):
        out = []
        for i in range(n_ctx):
            z, c = divmod(i, 2)
            step = {0: 0, 1: 1, 2: 2 - 4 * c, 3: -1}[k]
            out.append((i, 2 * ((z + step) % chips) + c))
        return out

    def partner(i, n, turn):
        return i ^ 1 if turn == 0 else (((i + 1) % n) ^ 1) - 1 if ((i + 1) % n) ^ 1 else n - 1

    near_pairs = [near_to(k) for k in range(radix)]
    far_pairs = [
        [
            (i, 2 * (partner(z // radix, far, t ^ c) * radix + z % radix) + c)
            for i in range(n_ctx)
            for z, c in [divmod(i, 2)]
        ]
        for t in range(2)
    ]
    n_head = lax.axis_size("head")
    head_pairs = [
        [
            (i * n_head + h, i * n_head + partner(h, n_head, t ^ (i % 2)))
            for i in range(n_ctx)
            for h in range(n_head)
        ]
        for t in range(2)
    ]
    core_pairs = [(i, i ^ 1) for i in range(n_ctx)]

    swap = lambda x: lax.ppermute(x, "ctx", core_pairs)
    to_near = lambda x, k: lax.ppermute(x, "ctx", near_pairs[k])
    to_far = lambda x, t: lax.ppermute(x, "ctx", far_pairs[t])
    to_head = lambda x, t: lax.ppermute(x, ("ctx", "head"), head_pairs[t])

    index = lax.axis_index("ctx")
    core = index % 2
    spot = index // 2 % radix
    info = jnp.concatenate([jnp.stack([index * ctx_len, spot, core]).astype(jnp.int32), lengths])

    grouped = query.reshape(seqs, heads, queries, head_dim)
    keys = key_cache.reshape(seqs, ctx_len * heads, head_dim)
    values = value_cache.reshape(seqs, ctx_len * heads, head_dim)
    chunk = jax.ShapeDtypeStruct((head_dim + stat_rows, queries), f32)
    steps = (2, 1, 3)
    pair, last = attend(grouped, keys, values, info, scaling, steps)
    chunks = {}
    gate = info
    for call, seqs_of in enumerate((steps, (0,))):
        mine, theirs = pair if call == 0 else last(gate)
        got = swap(theirs)
        found = pl.pallas_call(
            merge_core_kernel,
            in_specs=whole_vmem(2),
            out_specs=whole_vmem(len(seqs_of)),
            out_shape=[chunk] * len(seqs_of),
            name="merge_core",
            compiler_params=limit(8),
        )(mine, got)
        gate, *found = lax.optimization_barrier((info, *found))
        for k, x in zip(seqs_of, found):
            chunks[k] = to_near(x, k) if k else x
    chunks = [chunks[k] for k in range(radix)]
    half_chunk = jax.ShapeDtypeStruct((head_dim + stat_rows, queries // 2), f32)

    def merge(parts, n_out):
        return pl.pallas_call(
            functools.partial(merge_kernel, n_out),
            in_specs=whole_vmem(len(parts)),
            out_specs=whole_vmem(n_out),
            out_shape=[half_chunk] * n_out,
            name="merge",
            compiler_params=limit(4),
        )(*parts)

    found = merge(chunks, 2)
    own = pl.pallas_call(
        functools.partial(own_kernel, scaling, draft),
        in_specs=[smem] + whole_vmem(3),
        out_specs=whole_vmem(2),
        out_shape=[half_chunk] * 2,
        name="own",
        compiler_params=limit(4),
    )(info, grouped, new_key, new_value)
    width = out_weight.shape[1]
    found = [merge([x, to_far(x, 0)], 1)[0] for x in found]
    out = []
    for n, x in enumerate(found):
        parts = [x, to_far(x, 1), own[n]]
        att = pl.pallas_call(
            finish_kernel,
            in_specs=whole_vmem(len(parts)),
            out_specs=pl.BlockSpec(memory_space=VMEM),
            out_shape=jax.ShapeDtypeStruct((head_dim, queries // 2), f32),
            name="finish",
            compiler_params=limit(4),
        )(*parts)
        near = [att] + [to_near(att, radix - k) for k in range(1, radix)]
        pieces = []
        for part in near:
            pieces += [part, swap(part)]
        out = [
            pl.pallas_call(
                functools.partial(project_kernel, draft, n),
                in_specs=[smem] + whole_vmem(len(pieces) + len(out) + 1),
                out_specs=pl.BlockSpec(memory_space=VMEM),
                out_shape=jax.ShapeDtypeStruct((seqs * draft, width), f32),
                scratch_shapes=[
                    VMEM((heads, seqs * draft, out_weight.shape[0] // heads // 2), bf16)
                ],
                name="project",
                compiler_params=limit(8),
            )(info, *pieces, *out, out_weight)
        ]
    out = out[0]
    for t in range(2):
        out = out + to_head(out, t)
    return out.reshape(seqs, draft, width)


def solution(mesh):
    placed = (
        P("groups", "head", None, None),
        P("groups", "ctx", "head", None),
        P("groups", "ctx", "head", None),
        P("groups", "head", None, None),
        P("groups", "head", None, None),
        P("groups"),
        P("head", "ctx"),
    )
    return jax.shard_map(
        step, mesh=mesh, in_specs=placed, out_specs=P("groups", None, "ctx"), check_vma=False
    )
```

```python
import functools
import math

import jax
import jax.numpy as jnp
from jax import lax
from jax.experimental import pallas as pl
from jax.experimental.pallas import tpu as pltpu
from jax.sharding import PartitionSpec as P


very_low = -1e30
page = 256
radix = 4
stat_rows = 8

VMEM = pltpu.VMEM
f32 = jnp.float32
bf16 = jnp.bfloat16


def stats(top, total):
    row = lax.broadcasted_iota(jnp.int32, (stat_rows, top.shape[-1]), 0)
    return jnp.where(row == 0, top, jnp.where(row == 1, total, 0.0))


def contract(a, b, da, db, precision=None):
    return lax.dot_general(
        a, b, (((da,), (db,)), ((), ())), preferred_element_type=f32, precision=precision
    )


def attend_kernel(scaling, order, ahead, info, q_hbm, k_hbm, v_hbm, *refs):
    n_out = 2 + 3 * ahead
    mine_ref, theirs_ref, *next_refs = refs[:n_out]
    q_buf, k_buf, v_buf, s_ref, acc_ref, sems = refs[n_out:]
    steps = q_buf.shape[0]

    def usable(seq):
        return jnp.clip(info[3 + seq] - info[0], 0, k_buf.shape[1] // 2)

    def seq_of(i):
        return lax.rem(info[1] + order(i), radix)

    def copies(i, seq, bufs):
        return [
            pltpu.make_async_copy(hbm.at[seq], buf, sems.at[i, n])
            for n, (hbm, buf) in enumerate(zip((q_hbm, k_hbm, v_hbm), bufs))
        ]

    def slot(i):
        return copies(i, seq_of(i), (q_buf.at[i], k_buf.at[i], v_buf.at[i]))

    def begin(i):
        @pl.when(usable(seq_of(i)) > 0)
        def _():
            for copy in slot(i):
                copy.start()

    begin(0)
    if ahead:
        later = copies(steps, info[1], next_refs)

    def one(i, _):
        def then():
            @pl.when(i + 1 < steps)
            def _():
                begin(jnp.minimum(i + 1, steps - 1))

            if ahead:

                @pl.when(jnp.logical_and(i + 1 == steps, usable(info[1]) > 0))
                def _():
                    for copy in later:
                        copy.start()

        count = usable(seq_of(i))
        refs = (q_buf.at[i], k_buf.at[i], v_buf.at[i], mine_ref.at[i], theirs_ref.at[i])
        attend_one(scaling, info[2], count, slot(i), *refs, s_ref, acc_ref, then)
        return _

    lax.fori_loop(0, steps, one, 0)
    if ahead:

        @pl.when(usable(info[1]) > 0)
        def _():
            for copy in later:
                copy.wait()


def attend_last_kernel(scaling, info, q_ref, k_ref, v_ref, mine_ref, theirs_ref, s_ref, acc_ref):
    count = jnp.clip(info[3 + info[1]] - info[0], 0, k_ref.shape[0] // 2)
    refs = (q_ref, k_ref, v_ref, mine_ref.at[0], theirs_ref.at[0])
    attend_one(scaling, info[2], count, None, *refs, s_ref, acc_ref)


def attend_one(scaling, core, usable, copies, q_ref, k_ref, v_ref, mine_ref, theirs_ref, s_ref, acc_ref, then=None):
    rows, head_dim = k_ref.shape
    queries = q_ref.shape[1]
    per_page = 2 * page
    pages = usable // page
    some = pages > 0
    factor = scaling * math.log2(math.e)
    d2 = 2 * head_dim

    even_row = lax.broadcasted_iota(jnp.int32, (16, head_dim), 0) % 2 == 0
    pick_even = jnp.where(even_row, 1.0, 0.0).astype(bf16)
    pick_odd = jnp.where(even_row, 0.0, 1.0).astype(bf16)

    if copies:

        @pl.when(some)
        def _():
            copies[0].wait()
            copies[1].wait()

        then()

    qc = jnp.concatenate([q_ref[0].T, q_ref[1].T], axis=0)

    def scores(p, tile):
        k = k_ref[pl.ds(p * per_page, tile), :].reshape(tile // 16, 16, head_dim)
        wide = jnp.concatenate(
            [
                (k * pick_even[None]).reshape(tile, head_dim),
                (k * pick_odd[None]).reshape(tile, head_dim),
            ],
            axis=1,
        )
        s = contract(wide, qc, 1, 0)
        s_ref[pl.ds(p * per_page, tile), :] = s
        return jnp.max(s.reshape(tile // 8, 8, queries), axis=0)

    def tops(most):
        even = lax.broadcasted_iota(jnp.int32, (8, queries), 0) % 2 == 0
        low = jnp.full_like(most, -jnp.inf)
        top0 = jnp.max(jnp.where(even, most, low), axis=0, keepdims=True)
        top1 = jnp.max(jnp.where(even, low, most), axis=0, keepdims=True)
        return top0, top1, jnp.where(even, top0, top1)

    def weighted(p, tile, both):
        s = s_ref[pl.ds(p * per_page, tile), :].reshape(tile // 8, 8, queries)
        w = jnp.exp2((s - both[None]) * factor).reshape(tile, queries).astype(bf16)
        v = v_ref[pl.ds(p * per_page, tile), :].T
        even = lax.broadcasted_iota(jnp.int32, (16, tile), 1) % 2 == 0
        even_lane = jnp.where(even, 1.0, 0.0).astype(bf16)
        odd_lane = jnp.where(even, 0.0, 1.0).astype(bf16)
        first = lax.broadcasted_iota(jnp.int32, (16, tile), 0)
        ones = jnp.where(
            first == 0, even_lane.astype(f32), jnp.where(first == 1, odd_lane.astype(f32), 0.0)
        ).astype(bf16)
        v3 = v.reshape(head_dim // 16, 16, tile)
        wide = jnp.concatenate(
            [
                (v3 * even_lane[None]).reshape(head_dim, tile),
                (v3 * odd_lane[None]).reshape(head_dim, tile),
                ones,
            ],
            axis=0,
        )
        return contract(wide, w, 1, 0)

    whole = rows // per_page
    spans, start = [], jnp.int32(0)
    for run in (whole, whole // 2, 1):
        count = (pages - start) // run
        spans.append((run, start, count))
        start = start + count * run

    def look(p, count, most):
        for i in range(count):
            most = jnp.maximum(most, scores(p + i, per_page))
        return most

    most = jnp.full((8, queries), -jnp.inf, f32)
    for run, start, count in spans:
        most = lax.fori_loop(
            0, count, lambda i, m, run=run, start=start: look(start + i * run, run, m), most
        )
    top0, top1, both = tops(most)
    acc_ref[...] = jnp.zeros_like(acc_ref)

    if copies:

        @pl.when(some)
        def _():
            copies[2].wait()

    def add(p, count):
        acc_ref[...] += sum(weighted(p + i, per_page, both) for i in range(count))

    for run, start, count in spans:
        lax.fori_loop(
            0, count, lambda i, _, run=run, start=start: add(start + i * run, run), None
        )
    a0, a1 = acc_ref[:head_dim], acc_ref[head_dim:d2]
    s0 = stats(jnp.where(some, top0 * scaling, very_low), acc_ref[d2 : d2 + 1])
    s1 = stats(jnp.where(some, top1 * scaling, very_low), acc_ref[d2 + 1 : d2 + 2])
    first = core == 0
    mine_ref[:head_dim, :] = jnp.where(first, a0, a1)
    theirs_ref[:head_dim, :] = jnp.where(first, a1, a0)
    mine_ref[head_dim:, :] = jnp.where(first, s0, s1)
    theirs_ref[head_dim:, :] = jnp.where(first, s1, s0)


def attend(query, key_cache, value_cache, info, scaling, steps):
    _, heads, queries, head_dim = query.shape
    rows = key_cache.shape[1]
    block = (head_dim + stat_rows, queries)
    work = [VMEM((rows, queries), f32), VMEM((2 * head_dim + 16, queries), f32)]

    def cost(n):
        return pl.CostEstimate(
            flops=8 * n * rows * queries * head_dim,
            transcendentals=n * rows * queries,
            bytes_accessed=4 * n * rows * head_dim,
        )

    def outs(n):
        return [jax.ShapeDtypeStruct((n, *block), f32)] * 2

    def order(i):
        at = jnp.int32(steps[0])
        for n, k in enumerate(steps):
            at = jnp.where(i == n, k, at)
        return at

    n = len(steps)
    in_hbm = [pltpu.with_memory_space_constraint(x, pltpu.HBM) for x in (query, key_cache, value_cache)]
    *most, q, k, v = pl.pallas_call(
        functools.partial(attend_kernel, scaling, order, True),
        in_specs=[smem] + [pl.BlockSpec(memory_space=pltpu.HBM)] * 3,
        out_specs=whole_vmem(5),
        out_shape=outs(n)
        + [jax.ShapeDtypeStruct(x.shape[1:], x.dtype) for x in (query, key_cache, value_cache)],
        scratch_shapes=[
            VMEM((n, heads, queries, head_dim), bf16),
            VMEM((n, rows, head_dim), bf16),
            VMEM((n, rows, head_dim), bf16),
            *work,
            pltpu.SemaphoreType.DMA((n + 1, 3)),
        ],
        name="attend",
        compiler_params=limit(26),
        cost_estimate=cost(n),
    )(info, *in_hbm)

    def last(info):
        return pl.pallas_call(
            functools.partial(attend_last_kernel, scaling),
            in_specs=[smem] + whole_vmem(3),
            out_specs=whole_vmem(2),
            out_shape=outs(1),
            scratch_shapes=work,
            name="attend_last",
            compiler_params=limit(16),
            cost_estimate=cost(1),
        )(info, q, k, v)

    return most, last


def merged(parts, depth):
    tops = [p[depth : depth + 1] for p in parts]
    top = functools.reduce(jnp.maximum, tops)
    shares = [jnp.exp(t - top) for t in tops]
    numer = sum(p[:depth] * e for p, e in zip(parts, shares))
    total = sum(p[depth + 1 : depth + 2] * e for p, e in zip(parts, shares))
    return numer, top, total


def merge_core_kernel(mine_ref, got_ref, *outs):
    depth = mine_ref.shape[1] - stat_rows
    for k, out in enumerate(outs):
        numer, top, total = merged([mine_ref[k], got_ref[k]], depth)
        out[:depth, :] = numer
        out[depth:, :] = stats(top, total)


def merge_kernel(*refs):
    parts, out = refs[:-1], refs[-1]
    depth = out.shape[0] - stat_rows
    numer, top, total = merged([p[...] for p in parts], depth)
    out[:depth, :] = numer
    out[depth:, :] = stats(top, total)


def own_kernel(scaling, draft, info, q_ref, key_ref, value_ref, out):
    depth = out.shape[0] - stat_rows
    own = contract(key_ref[info[1], info[2]], q_ref[info[1], info[2]], 1, 1) * scaling
    at = lax.broadcasted_iota(jnp.int32, own.shape, 0)
    row = lax.broadcasted_iota(jnp.int32, own.shape, 1) % draft
    causal = at <= row
    own = jnp.where(causal, own, very_low)
    top = jnp.max(own, axis=0, keepdims=True)
    fresh = jnp.where(causal, jnp.exp(own - top), 0.0)
    values = value_ref[info[1], info[2]].astype(f32)
    out[:depth, :] = contract(values, fresh, 0, 0, lax.Precision.HIGHEST)
    out[depth:, :] = stats(top, jnp.sum(fresh, axis=0, keepdims=True))


def finish_kernel(*refs):
    parts, out = refs[:-1], refs[-1]
    numer, _, total = merged([p[...] for p in parts], out.shape[0])
    out[...] = (numer / total).astype(bf16).astype(f32)


def project_kernel(draft, info, *refs):
    pieces, (w_ref, out_ref, x_ref) = refs[:-3], refs[-3:]
    width = x_ref.shape[2]
    for i, piece in enumerate(pieces):
        k, other = i // 2, i % 2
        g = jnp.bitwise_xor(info[2], other)
        seq = lax.rem(info[1] + k, radix)
        at = pl.ds(pl.multiple_of(seq * draft, draft), draft)
        depth, queries = piece.shape
        for a in range(queries // depth):
            att = piece[:, a * depth : (a + 1) * depth].T.astype(bf16)
            for h in range(depth // draft):
                col = (a * (depth // draft) + h) * depth
                x_ref[g, at, col : col + depth] = att[h * draft : (h + 1) * draft]
    out_ref[...] = sum(contract(x_ref[g], w_ref[g * width : (g + 1) * width, :], 1, 0) for g in range(2))


def whole_vmem(n):
    return [pl.BlockSpec(memory_space=VMEM)] * n


def limit(mib):
    return pltpu.CompilerParams(vmem_limit_bytes=mib * 2**20)


smem = pl.BlockSpec(memory_space=pltpu.SMEM)


def step(query, key_cache, value_cache, new_key, new_value, lengths, out_weight):
    seqs, q_count, draft, head_dim = query.shape
    ctx_len, heads = key_cache.shape[1], key_cache.shape[2]
    queries = q_count // heads * draft
    scaling = 1.0 / math.sqrt(head_dim)
    n_ctx = lax.axis_size("ctx")
    chips = n_ctx // 2
    far = chips // radix

    def near_to(k):
        out = []
        for i in range(n_ctx):
            z, c = divmod(i, 2)
            step = {0: 0, 1: 1, 2: 2 - 4 * c, 3: -1}[k]
            out.append((i, 2 * ((z + step) % chips) + c))
        return out

    def partner(i, n, turn):
        return i ^ 1 if turn == 0 else (((i + 1) % n) ^ 1) - 1 if ((i + 1) % n) ^ 1 else n - 1

    near_pairs = [near_to(k) for k in range(radix)]
    far_pairs = [
        [
            (i, 2 * (partner(z // radix, far, t ^ c) * radix + z % radix) + c)
            for i in range(n_ctx)
            for z, c in [divmod(i, 2)]
        ]
        for t in range(2)
    ]
    n_head = lax.axis_size("head")
    head_pairs = [
        [
            (i * n_head + h, i * n_head + partner(h, n_head, t ^ (i % 2)))
            for i in range(n_ctx)
            for h in range(n_head)
        ]
        for t in range(2)
    ]
    core_pairs = [(i, i ^ 1) for i in range(n_ctx)]

    swap = lambda x: lax.ppermute(x, "ctx", core_pairs)
    to_near = lambda x, k: lax.ppermute(x, "ctx", near_pairs[k])
    to_far = lambda x, t: lax.ppermute(x, "ctx", far_pairs[t])
    to_head = lambda x, t: lax.ppermute(x, ("ctx", "head"), head_pairs[t])

    index = lax.axis_index("ctx")
    core = index % 2
    spot = index // 2 % radix
    info = jnp.concatenate([jnp.stack([index * ctx_len, spot, core]).astype(jnp.int32), lengths])

    grouped = query.reshape(seqs, heads, queries, head_dim)
    keys = key_cache.reshape(seqs, ctx_len * heads, head_dim)
    values = value_cache.reshape(seqs, ctx_len * heads, head_dim)
    chunk = jax.ShapeDtypeStruct((head_dim + stat_rows, queries), f32)
    steps = (2, 1, 3)
    pair, last = attend(grouped, keys, values, info, scaling, steps)
    chunks = {}
    gate = info
    for call, seqs_of in enumerate((steps, (0,))):
        mine, theirs = pair if call == 0 else last(gate)
        got = swap(theirs)
        found = pl.pallas_call(
            merge_core_kernel,
            in_specs=whole_vmem(2),
            out_specs=whole_vmem(len(seqs_of)),
            out_shape=[chunk] * len(seqs_of),
            name="merge_core",
            compiler_params=limit(8),
        )(mine, got)
        gate, *found = lax.optimization_barrier((info, *found))
        for k, x in zip(seqs_of, found):
            chunks[k] = to_near(x, k) if k else x
    chunks = [chunks[k] for k in range(radix)]

    def merge(parts):
        return pl.pallas_call(
            merge_kernel,
            in_specs=whole_vmem(len(parts)),
            out_specs=pl.BlockSpec(memory_space=VMEM),
            out_shape=chunk,
            name="merge",
            compiler_params=limit(4),
        )(*parts)

    found = merge(chunks)
    found = merge([found, to_far(found, 0)])
    own = pl.pallas_call(
        functools.partial(own_kernel, scaling, draft),
        in_specs=[smem] + whole_vmem(3),
        out_specs=pl.BlockSpec(memory_space=VMEM),
        out_shape=chunk,
        name="own",
        compiler_params=limit(4),
    )(info, grouped, new_key, new_value)
    parts = [found, to_far(found, 1), own]
    att = pl.pallas_call(
        finish_kernel,
        in_specs=whole_vmem(len(parts)),
        out_specs=pl.BlockSpec(memory_space=VMEM),
        out_shape=jax.ShapeDtypeStruct((head_dim, queries), f32),
        name="finish",
        compiler_params=limit(4),
    )(*parts)
    near = [att] + [to_near(att, radix - k) for k in range(1, radix)]
    pieces = []
    for part in near:
        pieces += [part, swap(part)]
    width = out_weight.shape[1]
    out = pl.pallas_call(
        functools.partial(project_kernel, draft),
        in_specs=[smem] + whole_vmem(len(pieces) + 1),
        out_specs=pl.BlockSpec(memory_space=VMEM),
        out_shape=jax.ShapeDtypeStruct((seqs * draft, width), f32),
        scratch_shapes=[VMEM((heads, seqs * draft, out_weight.shape[0] // heads), bf16)],
        name="project",
        compiler_params=limit(8),
    )(info, *pieces, out_weight)
    for t in range(2):
        out = out + to_head(out, t)
    return out.reshape(seqs, draft, width)


def solution(mesh):
    placed = (
        P("groups", "head", None, None),
        P("groups", "ctx", "head", None),
        P("groups", "ctx", "head", None),
        P("groups", "head", None, None),
        P("groups", "head", None, None),
        P("groups"),
        P("head", "ctx"),
    )
    return jax.shard_map(
        step, mesh=mesh, in_specs=placed, out_specs=P("groups", None, "ctx"), check_vma=False
    )
```

```python
import functools
import math

import jax
import jax.numpy as jnp
from jax import lax
from jax.experimental import pallas as pl
from jax.experimental.pallas import tpu as pltpu
from jax.sharding import PartitionSpec as P


very_low = -1e30
page = 256
radix = 4
stat_rows = 8

VMEM = pltpu.VMEM
f32 = jnp.float32
bf16 = jnp.bfloat16


def stats(top, total):
    row = lax.broadcasted_iota(jnp.int32, (stat_rows, top.shape[-1]), 0)
    return jnp.where(row == 0, top, jnp.where(row == 1, total, 0.0))


def contract(a, b, da, db, precision=None):
    return lax.dot_general(
        a, b, (((da,), (db,)), ((), ())), preferred_element_type=f32, precision=precision
    )


def attend_kernel(scaling, order, ahead, info, q_hbm, k_hbm, v_hbm, *refs):
    n_out = 2 + 3 * ahead
    mine_ref, theirs_ref, *next_refs = refs[:n_out]
    q_buf, k_buf, v_buf, s_ref, acc_ref, sems = refs[n_out:]
    steps = q_buf.shape[0]

    def usable(seq):
        return jnp.clip(info[3 + seq] - info[0], 0, k_buf.shape[1] // 2)

    def seq_of(i):
        return lax.rem(info[1] + order(i), radix)

    def copies(i, seq, bufs):
        return [
            pltpu.make_async_copy(hbm.at[seq], buf, sems.at[i, n])
            for n, (hbm, buf) in enumerate(zip((q_hbm, k_hbm, v_hbm), bufs))
        ]

    def slot(i):
        return copies(i, seq_of(i), (q_buf.at[i], k_buf.at[i], v_buf.at[i]))

    def begin(i):
        @pl.when(usable(seq_of(i)) > 0)
        def _():
            for copy in slot(i):
                copy.start()

    begin(0)
    if ahead:
        later = copies(steps, info[1], next_refs)

    def one(i, _):
        def then():
            @pl.when(i + 1 < steps)
            def _():
                begin(jnp.minimum(i + 1, steps - 1))

            if ahead:

                @pl.when(jnp.logical_and(i + 1 == steps, usable(info[1]) > 0))
                def _():
                    for copy in later:
                        copy.start()

        count = usable(seq_of(i))
        refs = (q_buf.at[i], k_buf.at[i], v_buf.at[i], mine_ref.at[i], theirs_ref.at[i])
        attend_one(scaling, info[2], count, slot(i), *refs, s_ref, acc_ref, then)
        return _

    lax.fori_loop(0, steps, one, 0)
    if ahead:

        @pl.when(usable(info[1]) > 0)
        def _():
            for copy in later:
                copy.wait()


def attend_last_kernel(scaling, info, q_ref, k_ref, v_ref, mine_ref, theirs_ref, s_ref, acc_ref):
    count = jnp.clip(info[3 + info[1]] - info[0], 0, k_ref.shape[0] // 2)
    refs = (q_ref, k_ref, v_ref, mine_ref.at[0], theirs_ref.at[0])
    attend_one(scaling, info[2], count, None, *refs, s_ref, acc_ref)


def attend_one(scaling, core, usable, copies, q_ref, k_ref, v_ref, mine_ref, theirs_ref, s_ref, acc_ref, then=None):
    rows, head_dim = k_ref.shape
    queries = q_ref.shape[1]
    per_page = 2 * page
    pages = usable // page
    some = pages > 0
    factor = scaling * math.log2(math.e)
    d2 = 2 * head_dim

    even_row = lax.broadcasted_iota(jnp.int32, (16, head_dim), 0) % 2 == 0
    pick_even = jnp.where(even_row, 1.0, 0.0).astype(bf16)
    pick_odd = jnp.where(even_row, 0.0, 1.0).astype(bf16)

    if copies:

        @pl.when(some)
        def _():
            copies[0].wait()
            copies[1].wait()

        then()

    qc = jnp.concatenate([q_ref[0].T, q_ref[1].T], axis=0)

    def scores(p, tile):
        k = k_ref[pl.ds(p * per_page, tile), :].reshape(tile // 16, 16, head_dim)
        wide = jnp.concatenate(
            [
                (k * pick_even[None]).reshape(tile, head_dim),
                (k * pick_odd[None]).reshape(tile, head_dim),
            ],
            axis=1,
        )
        s = contract(wide, qc, 1, 0)
        s_ref[pl.ds(p * per_page, tile), :] = s
        return jnp.max(s.reshape(tile // 8, 8, queries), axis=0)

    def tops(most):
        even = lax.broadcasted_iota(jnp.int32, (8, queries), 0) % 2 == 0
        low = jnp.full_like(most, -jnp.inf)
        top0 = jnp.max(jnp.where(even, most, low), axis=0, keepdims=True)
        top1 = jnp.max(jnp.where(even, low, most), axis=0, keepdims=True)
        return top0, top1, jnp.where(even, top0, top1)

    def weighted(p, tile, both):
        s = s_ref[pl.ds(p * per_page, tile), :].reshape(tile // 8, 8, queries)
        w = jnp.exp2((s - both[None]) * factor).reshape(tile, queries).astype(bf16)
        v = v_ref[pl.ds(p * per_page, tile), :].T
        even = lax.broadcasted_iota(jnp.int32, (16, tile), 1) % 2 == 0
        even_lane = jnp.where(even, 1.0, 0.0).astype(bf16)
        odd_lane = jnp.where(even, 0.0, 1.0).astype(bf16)
        first = lax.broadcasted_iota(jnp.int32, (16, tile), 0)
        ones = jnp.where(
            first == 0, even_lane.astype(f32), jnp.where(first == 1, odd_lane.astype(f32), 0.0)
        ).astype(bf16)
        v3 = v.reshape(head_dim // 16, 16, tile)
        wide = jnp.concatenate(
            [
                (v3 * even_lane[None]).reshape(head_dim, tile),
                (v3 * odd_lane[None]).reshape(head_dim, tile),
                ones,
            ],
            axis=0,
        )
        return contract(wide, w, 1, 0)

    whole = rows // per_page
    spans, start = [], jnp.int32(0)
    for run in (whole, whole // 2, 1):
        count = (pages - start) // run
        spans.append((run, start, count))
        start = start + count * run

    def look(p, count, most):
        for i in range(count):
            most = jnp.maximum(most, scores(p + i, per_page))
        return most

    most = jnp.full((8, queries), -jnp.inf, f32)
    for run, start, count in spans:
        most = lax.fori_loop(
            0, count, lambda i, m, run=run, start=start: look(start + i * run, run, m), most
        )
    top0, top1, both = tops(most)
    acc_ref[...] = jnp.zeros_like(acc_ref)

    if copies:

        @pl.when(some)
        def _():
            copies[2].wait()

    def add(p, count):
        acc_ref[...] += sum(weighted(p + i, per_page, both) for i in range(count))

    for run, start, count in spans:
        lax.fori_loop(
            0, count, lambda i, _, run=run, start=start: add(start + i * run, run), None
        )
    a0, a1 = acc_ref[:head_dim], acc_ref[head_dim:d2]
    s0 = stats(jnp.where(some, top0 * scaling, very_low), acc_ref[d2 : d2 + 1])
    s1 = stats(jnp.where(some, top1 * scaling, very_low), acc_ref[d2 + 1 : d2 + 2])
    first = core == 0
    mine_ref[:head_dim, :] = jnp.where(first, a0, a1)
    theirs_ref[:head_dim, :] = jnp.where(first, a1, a0)
    mine_ref[head_dim:, :] = jnp.where(first, s0, s1)
    theirs_ref[head_dim:, :] = jnp.where(first, s1, s0)


def attend(query, key_cache, value_cache, info, scaling, steps):
    _, heads, queries, head_dim = query.shape
    rows = key_cache.shape[1]
    block = (head_dim + stat_rows, queries)
    work = [VMEM((rows, queries), f32), VMEM((2 * head_dim + 16, queries), f32)]

    def cost(n):
        return pl.CostEstimate(
            flops=8 * n * rows * queries * head_dim,
            transcendentals=n * rows * queries,
            bytes_accessed=4 * n * rows * head_dim,
        )

    def outs(n):
        return [jax.ShapeDtypeStruct((n, *block), f32)] * 2

    def order(i):
        at = jnp.int32(steps[0])
        for n, k in enumerate(steps):
            at = jnp.where(i == n, k, at)
        return at

    n = len(steps)
    in_hbm = [pltpu.with_memory_space_constraint(x, pltpu.HBM) for x in (query, key_cache, value_cache)]
    *most, q, k, v = pl.pallas_call(
        functools.partial(attend_kernel, scaling, order, True),
        in_specs=[smem] + [pl.BlockSpec(memory_space=pltpu.HBM)] * 3,
        out_specs=whole_vmem(5),
        out_shape=outs(n)
        + [jax.ShapeDtypeStruct(x.shape[1:], x.dtype) for x in (query, key_cache, value_cache)],
        scratch_shapes=[
            VMEM((n, heads, queries, head_dim), bf16),
            VMEM((n, rows, head_dim), bf16),
            VMEM((n, rows, head_dim), bf16),
            *work,
            pltpu.SemaphoreType.DMA((n + 1, 3)),
        ],
        name="attend",
        compiler_params=limit(26),
        cost_estimate=cost(n),
    )(info, *in_hbm)

    def last(info):
        return pl.pallas_call(
            functools.partial(attend_last_kernel, scaling),
            in_specs=[smem] + whole_vmem(3),
            out_specs=whole_vmem(2),
            out_shape=outs(1),
            scratch_shapes=work,
            name="attend_last",
            compiler_params=limit(16),
            cost_estimate=cost(1),
        )(info, q, k, v)

    return most, last


def merged(parts, depth):
    tops = [p[depth : depth + 1] for p in parts]
    top = functools.reduce(jnp.maximum, tops)
    shares = [jnp.exp(t - top) for t in tops]
    numer = sum(p[:depth] * e for p, e in zip(parts, shares))
    total = sum(p[depth + 1 : depth + 2] * e for p, e in zip(parts, shares))
    return numer, top, total


def merge_core_kernel(mine_ref, got_ref, *outs):
    depth = mine_ref.shape[1] - stat_rows
    for k, out in enumerate(outs):
        numer, top, total = merged([mine_ref[k], got_ref[k]], depth)
        out[:depth, :] = numer
        out[depth:, :] = stats(top, total)


def put_halves(outs, numer, top, total):
    depth, lanes = numer.shape[0], outs[0].shape[1]
    for n, out in enumerate(outs):
        at = slice(n * lanes, (n + 1) * lanes)
        out[:depth, :] = numer[:, at]
        out[depth:, :] = stats(top[:, at], total[:, at])


def merge_kernel(n_out, *refs):
    parts, outs = refs[:-n_out], refs[-n_out:]
    put_halves(outs, *merged([p[...] for p in parts], outs[0].shape[0] - stat_rows))


def own_kernel(scaling, draft, info, q_ref, key_ref, value_ref, *outs):
    own = contract(key_ref[info[1], info[2]], q_ref[info[1], info[2]], 1, 1) * scaling
    at = lax.broadcasted_iota(jnp.int32, own.shape, 0)
    row = lax.broadcasted_iota(jnp.int32, own.shape, 1) % draft
    causal = at <= row
    own = jnp.where(causal, own, very_low)
    top = jnp.max(own, axis=0, keepdims=True)
    fresh = jnp.where(causal, jnp.exp(own - top), 0.0)
    values = value_ref[info[1], info[2]].astype(f32)
    numer = contract(values, fresh, 0, 0, lax.Precision.HIGHEST)
    put_halves(outs, numer, top, jnp.sum(fresh, axis=0, keepdims=True))


def finish_kernel(*refs):
    parts, out = refs[:-1], refs[-1]
    numer, _, total = merged([p[...] for p in parts], out.shape[0])
    out[...] = (numer / total).astype(bf16).astype(f32)


def project_kernel(draft, half, info, *refs):
    n = 2 * radix
    pieces, extra, (w_ref, out_ref, x_ref) = refs[:n], refs[n:-3], refs[-3:]
    width = x_ref.shape[2]
    for i, piece in enumerate(pieces):
        k, other = i // 2, i % 2
        g = jnp.bitwise_xor(info[2], other)
        seq = lax.rem(info[1] + k, radix)
        at = pl.ds(pl.multiple_of(seq * draft, draft), draft)
        depth, lanes = piece.shape
        att = piece[...].T.astype(bf16)
        for h in range(lanes // draft):
            x_ref[g, at, h * depth : (h + 1) * depth] = att[h * draft : (h + 1) * draft]
    whole = w_ref.shape[0] // 2
    products = [
        contract(x_ref[g], w_ref[g * whole + half * width : g * whole + (half + 1) * width, :], 1, 0)
        for g in range(2)
    ]
    out_ref[...] = sum(products + [e[...] for e in extra])


def whole_vmem(n):
    return [pl.BlockSpec(memory_space=VMEM)] * n


def limit(mib):
    return pltpu.CompilerParams(vmem_limit_bytes=mib * 2**20)


smem = pl.BlockSpec(memory_space=pltpu.SMEM)


def step(query, key_cache, value_cache, new_key, new_value, lengths, out_weight):
    seqs, q_count, draft, head_dim = query.shape
    ctx_len, heads = key_cache.shape[1], key_cache.shape[2]
    queries = q_count // heads * draft
    scaling = 1.0 / math.sqrt(head_dim)
    n_ctx = lax.axis_size("ctx")
    chips = n_ctx // 2
    far = chips // radix

    def near_to(k):
        out = []
        for i in range(n_ctx):
            z, c = divmod(i, 2)
            step = {0: 0, 1: 1, 2: 2 - 4 * c, 3: -1}[k]
            out.append((i, 2 * ((z + step) % chips) + c))
        return out

    def partner(i, n, turn):
        return i ^ 1 if turn == 0 else (((i + 1) % n) ^ 1) - 1 if ((i + 1) % n) ^ 1 else n - 1

    near_pairs = [near_to(k) for k in range(radix)]
    far_pairs = [
        [
            (i, 2 * (partner(z // radix, far, t ^ c) * radix + z % radix) + c)
            for i in range(n_ctx)
            for z, c in [divmod(i, 2)]
        ]
        for t in range(2)
    ]
    n_head = lax.axis_size("head")
    head_pairs = [
        [
            (i * n_head + h, i * n_head + partner(h, n_head, t ^ (i % 2)))
            for i in range(n_ctx)
            for h in range(n_head)
        ]
        for t in range(2)
    ]
    core_pairs = [(i, i ^ 1) for i in range(n_ctx)]

    swap = lambda x: lax.ppermute(x, "ctx", core_pairs)
    to_near = lambda x, k: lax.ppermute(x, "ctx", near_pairs[k])
    to_far = lambda x, t: lax.ppermute(x, "ctx", far_pairs[t])
    to_head = lambda x, t: lax.ppermute(x, ("ctx", "head"), head_pairs[t])

    index = lax.axis_index("ctx")
    core = index % 2
    spot = index // 2 % radix
    info = jnp.concatenate([jnp.stack([index * ctx_len, spot, core]).astype(jnp.int32), lengths])

    grouped = query.reshape(seqs, heads, queries, head_dim)
    keys = key_cache.reshape(seqs, ctx_len * heads, head_dim)
    values = value_cache.reshape(seqs, ctx_len * heads, head_dim)
    chunk = jax.ShapeDtypeStruct((head_dim + stat_rows, queries), f32)
    steps = (2, 1, 3)
    pair, last = attend(grouped, keys, values, info, scaling, steps)
    chunks = {}
    for call, seqs_of in enumerate((steps, (0,))):
        mine, theirs = pair if call == 0 else last(info)
        got = swap(theirs)
        found = pl.pallas_call(
            merge_core_kernel,
            in_specs=whole_vmem(2),
            out_specs=whole_vmem(len(seqs_of)),
            out_shape=[chunk] * len(seqs_of),
            name="merge_core",
            compiler_params=limit(8),
        )(mine, got)
        for k, x in zip(seqs_of, found):
            chunks[k] = to_near(x, k) if k else x
    chunks = [chunks[k] for k in range(radix)]
    half_chunk = jax.ShapeDtypeStruct((head_dim + stat_rows, queries // 2), f32)

    def merge(parts, n_out):
        return pl.pallas_call(
            functools.partial(merge_kernel, n_out),
            in_specs=whole_vmem(len(parts)),
            out_specs=whole_vmem(n_out),
            out_shape=[half_chunk] * n_out,
            name="merge",
            compiler_params=limit(4),
        )(*parts)

    found = merge(chunks, 2)
    own = pl.pallas_call(
        functools.partial(own_kernel, scaling, draft),
        in_specs=[smem] + whole_vmem(3),
        out_specs=whole_vmem(2),
        out_shape=[half_chunk] * 2,
        name="own",
        compiler_params=limit(4),
    )(info, grouped, new_key, new_value)
    width = out_weight.shape[1]
    found = [merge([x, to_far(x, 0)], 1)[0] for x in found]
    out = []
    for n, x in enumerate(found):
        parts = [x, to_far(x, 1), own[n]]
        att = pl.pallas_call(
            finish_kernel,
            in_specs=whole_vmem(len(parts)),
            out_specs=pl.BlockSpec(memory_space=VMEM),
            out_shape=jax.ShapeDtypeStruct((head_dim, queries // 2), f32),
            name="finish",
            compiler_params=limit(4),
        )(*parts)
        near = [att] + [to_near(att, radix - k) for k in range(1, radix)]
        pieces = []
        for part in near:
            pieces += [part, swap(part)]
        out = [
            pl.pallas_call(
                functools.partial(project_kernel, draft, n),
                in_specs=[smem] + whole_vmem(len(pieces) + len(out) + 1),
                out_specs=pl.BlockSpec(memory_space=VMEM),
                out_shape=jax.ShapeDtypeStruct((seqs * draft, width), f32),
                scratch_shapes=[
                    VMEM((heads, seqs * draft, out_weight.shape[0] // heads // 2), bf16)
                ],
                name="project",
                compiler_params=limit(8),
            )(info, *pieces, *out, out_weight)
        ]
    out = out[0]
    for t in range(2):
        out = out + to_head(out, t)
    return out.reshape(seqs, draft, width)


def solution(mesh):
    placed = (
        P("groups", "head", None, None),
        P("groups", "ctx", "head", None),
        P("groups", "ctx", "head", None),
        P("groups", "head", None, None),
        P("groups", "head", None, None),
        P("groups"),
        P("head", "ctx"),
    )
    return jax.shard_map(
        step, mesh=mesh, in_specs=placed, out_specs=P("groups", None, "ctx"), check_vma=False
    )
```
